256 devices in a mesh: src: 8 (over y, x_lo), tx: 8 (over z), ty: 4 (over x_hi, core).
Axes of the slice: x: 4 (x_hi: 2, x_lo: 2; x = x_hi * 2 + x_lo), y: 4, z: 8, core: 2. Of those that a mesh axis runs over, the one named last changes fastest.
Arguments:
- spectra: bfloat16 [32, 3, 2, 256, 256], P('src'), may hold values from -2.5 to 2.5
- pupil_shift: int32 [32, 2], P('src'), may hold values from -121 to 121
- window_offset: int32 [32, 2], P('src'), may hold values from -3 to 3
- source_weight: float32 [32], replicated, may hold values from 0.3 to 3
- mask_codes: int32 [128, 128], replicated, may hold values from 0 to 3
- levels: float32 [2, 4], replicated, may hold values from -1 to 1
- quench_start: float32 [512, 16, 512], P(('src', 'tx'), None, 'ty'), may hold values from 0.4 to 1.2
Outputs:
- acid: float32 [512, 16, 512], P(('src', 'tx'), None, 'ty')
- quencher: float32 [512, 16, 512], P(('src', 'tx'), None, 'ty')
- inhibitor: float32 [512, 16, 512], P(('src', 'tx'), None, 'ty')
The draws below stay inside these ranges and needn't reach their ends.
All inputs are finite; a program needn't handle non-finite values.
Results may differ from the reference program's by a relative error of at most 0.0014.
Values may be sent and summed in bfloat16 or wider, within the bound.
A program may use at most 128 MiB of HBM per device.

```python
import math
import jax
import jax.numpy as jnp
from jax import lax

WIN = 256
RADIUS = 124
CELL = 4
LEVELS = 4
STEPS = 8
DEPTH = 16
SOURCES = 32
NX = 512
NY = 512


def plant(entries, own_key, least, top_value):
    shape = entries.shape
    index_at = [jax.random.randint(jax.random.fold_in(own_key, axis), (), 0, shape[axis]) for axis in range(len(shape))]
    entries = entries.at[tuple(index_at)].set(least)
    longest = shape.index(max(shape))
    index_at[longest] = (index_at[longest] + 1) % shape[longest]
    return entries.at[tuple(index_at)].set(top_value)


def level_of(own_key, dims, split, low, high):
    level, own = 1.0, jax.random.fold_in(own_key, 6)
    for axis_at, blocks in split:
        steps = jnp.exp(jax.random.uniform(jax.random.fold_in(own, axis_at), (blocks,), jnp.float32, low / len(split), high / len(split)))
        level = level * jnp.repeat(steps, dims[axis_at] // blocks).reshape([-1 if axis == axis_at else 1 for axis in range(len(dims))])
    return level


def bell_draw(own_key, extent, deviation, bound, cuts=(), kind=jnp.bfloat16):
    drawn = deviation * jax.random.normal(own_key, extent, jnp.float32)
    if cuts:
        drawn = drawn * level_of(own_key, extent, cuts, -0.22, 0.18)
    return jnp.clip(drawn, -bound, bound).astype(kind)


def setup_inputs(seed: int = 0) -> dict:
    key_list = jax.random.split(jax.random.key(seed), 8)
    return {
        "spectra": bell_draw(key_list[0], (SOURCES, 3, 2, WIN, WIN), 0.4, 2.5, ((0, 8),)),
        "pupil_shift": plant(jax.random.randint(key_list[1], (SOURCES, 2), 3 - RADIUS, RADIUS - 2), jax.random.fold_in(key_list[1], 1), 3 - RADIUS, (RADIUS - 2) - 1).astype(jnp.int32),
        "window_offset": plant(jax.random.randint(key_list[2], (SOURCES, 2), RADIUS + 1 - WIN // 2, WIN // 2 - RADIUS), jax.random.fold_in(key_list[2], 1), RADIUS + 1 - WIN // 2, (WIN // 2 - RADIUS) - 1).astype(jnp.int32),
        "source_weight": jnp.clip(jnp.exp(jax.random.uniform(key_list[3], (SOURCES,), jnp.float32, math.log(0.3), math.log(3.0))), 0.3, 3.0),
        "mask_codes": plant(jax.random.randint(key_list[4], (NX // CELL, NY // CELL), 0, LEVELS), jax.random.fold_in(key_list[4], 1), 0, LEVELS - 1).astype(jnp.int32),
        "levels": jnp.clip(jax.random.uniform(key_list[5], (2, LEVELS), jnp.float32, -1.0, 1.0), -1.0, 1.0),
        "quench_start": jnp.clip(0.4 + 0.800000042 * jax.random.uniform(key_list[6], (NX, DEPTH, NY), jnp.float32) ** level_of(key_list[6], (NX, DEPTH, NY), ((0, 64), (2, 4)), -0.2, 0.2), 0.4, 1.2),
    }


TWO_PI = 2.0 * math.pi
NUM_AP = 0.33
DZ_WAVE = 0.148
ABSORB = 0.05
LATERAL_RATE = (0.2, 0.06)
DEPTH_RATE = (0.05, 0.015)
NEUTRAL = 0.08
DEPROTECT = 0.25

def cos_sin(numer, period):
    angle = TWO_PI / period * jnp.mod(numer, period).astype(jnp.float32)
    return (jnp.cos(angle), jnp.sin(angle))

def cell_table(orders, period, cell, count):
    within = jnp.arange(cell, dtype=jnp.int32)
    inner_cos, inner_sin = cos_sin(orders[:, None] * within[None, :], period)
    shape_re = lax.optimization_barrier(jnp.sum(inner_cos, axis=1)) / period
    shape_im = -lax.optimization_barrier(jnp.sum(inner_sin, axis=1)) / period
    corners = jnp.arange(count, dtype=jnp.int32) * cell
    edge_cos, edge_sin = cos_sin(orders[:, None] * corners[None, :], period)
    table_re = shape_re[:, None] * edge_cos + shape_im[:, None] * edge_sin
    table_im = shape_im[:, None] * edge_cos - shape_re[:, None] * edge_sin
    return (table_re, table_im)

def level_grid(mask_codes, levels):
    level_ids = jnp.arange(levels.shape[1], dtype=jnp.int32)
    onehot = (mask_codes[:, :, None] == level_ids[None, None, :]).astype(jnp.float32)
    return (lax.optimization_barrier(jnp.sum(onehot * levels[0], axis=2)), lax.optimization_barrier(jnp.sum(onehot * levels[1], axis=2)))

def product(left, right):
    return jnp.dot(left, right, precision=lax.Precision.HIGHEST, preferred_element_type=jnp.float32)

def mask_spectrum(orders_x, orders_y, grid_re, grid_im, period_x, period_y):
    kx_re, kx_im = cell_table(orders_x, period_x, CELL, grid_re.shape[0])
    ky_re, ky_im = cell_table(orders_y, period_y, CELL, grid_re.shape[1])
    half_re = product(grid_re, ky_re.T) - product(grid_im, ky_im.T)
    half_im = product(grid_re, ky_im.T) + product(grid_im, ky_re.T)
    spec_re = product(kx_re, half_re) - product(kx_im, half_im)
    spec_im = product(kx_re, half_im) + product(kx_im, half_re)
    return (spec_re, spec_im)

def window_spectrum(table, orders_x, orders_y, period_x, period_y):
    rows = jnp.take(table, jnp.mod(orders_x, period_x).astype(jnp.int32), axis=0)
    return jnp.take(rows, jnp.mod(orders_y, period_y).astype(jnp.int32), axis=1)

def window_orders(shift, offset, window):
    steps_in = jnp.arange(window, dtype=jnp.int32)
    orders_x = steps_in - shift[0] - window // 2 + offset[0]
    orders_y = steps_in - shift[1] - window // 2 + offset[1]
    return (orders_x, orders_y)

def source_operand(factor, thin_re, thin_im, orders_x, orders_y, shift, layers):
    factor_f = factor.astype(jnp.float32)
    spec_re = thin_re * factor_f[:, 0] - thin_im * factor_f[:, 1]
    spec_im = thin_re * factor_f[:, 1] + thin_im * factor_f[:, 0]
    freq_x = orders_x + shift[0]
    freq_y = orders_y + shift[1]
    radial = freq_x[:, None] * freq_x[:, None] + freq_y[None, :] * freq_y[None, :]
    inside = (radial <= RADIUS * RADIUS).astype(jnp.float32)
    bounded = jnp.minimum(radial, RADIUS * RADIUS).astype(jnp.float32)
    axial = jnp.sqrt(1.0 - (NUM_AP / RADIUS) ** 2 * bounded)
    heights = (jnp.arange(layers, dtype=jnp.float32) + 0.5) * (TWO_PI * DZ_WAVE)
    phase = heights[:, None, None] * (axial - 1.0)[None]
    rot_re = jnp.cos(phase) * inside
    rot_im = jnp.sin(phase) * inside
    op_re = spec_re[None] * rot_re[:, None] - spec_im[None] * rot_im[:, None]
    op_im = spec_re[None] * rot_im[:, None] + spec_im[None] * rot_re[:, None]
    return jnp.concatenate([op_re, op_im], axis=2).astype(jnp.bfloat16)

def row_table(orders_x, rows_x, period):
    cosine, sine = cos_sin(rows_x[:, None] * orders_x[None, :], period)
    upper = jnp.concatenate([cosine, -sine], axis=1)
    lower = jnp.concatenate([sine, cosine], axis=1)
    return jnp.stack([upper, lower], axis=1).astype(jnp.bfloat16)

def column_table(orders_y, cols_y, period):
    cosine, sine = cos_sin(orders_y[:, None] * cols_y[None, :], period)
    first = jnp.concatenate([cosine, sine], axis=1)
    second = jnp.concatenate([-sine, cosine], axis=1)
    return jnp.concatenate([first, second], axis=0).astype(jnp.bfloat16)

def source_image(operand, left, right):
    halves = jnp.einsum('rpk,zckq->rzcpq', left.astype(jnp.float32), operand.astype(jnp.float32)).astype(jnp.bfloat16)
    merged = halves.reshape(halves.shape[:3] + (-1,))
    waves = jnp.einsum('rzcm,mn->rzcn', merged.astype(jnp.float32), right.astype(jnp.float32))
    power = lax.optimization_barrier(jnp.sum(waves * waves, axis=2))
    columns = power.shape[2] // 2
    return power[:, :, :columns] + power[:, :, columns:]

def evolve(centre, beside_all):
    above = jnp.concatenate([centre[:, :, :1], centre[:, :, :-1]], axis=2)
    below = jnp.concatenate([centre[:, :, 1:], centre[:, :, -1:]], axis=2)
    lateral = jnp.asarray(LATERAL_RATE, jnp.float32)[None, :, None, None]
    vertical = jnp.asarray(DEPTH_RATE, jnp.float32)[None, :, None, None]
    change = lateral * (beside_all - 4.0 * centre) + vertical * (above + below - 2.0 * centre)
    reaction = NEUTRAL * centre[:, 0] * centre[:, 1]
    return centre + change - reaction[:, None]

def reference(spectra, pupil_shift, window_offset, source_weight, mask_codes, levels, quench_start):
    grid_re, grid_im = level_grid(mask_codes, levels)
    rows_x = jnp.arange(NX, dtype=jnp.int32)
    cols_y = jnp.arange(NY, dtype=jnp.int32)
    table_re, table_im = mask_spectrum(rows_x, cols_y, grid_re, grid_im, NX, NY)

    def add_source(total, pieces):
        factor, shift, offset, weight = pieces
        orders_x, orders_y = window_orders(shift, offset, WIN)
        thin_re = window_spectrum(table_re, orders_x, orders_y, NX, NY)
        thin_im = window_spectrum(table_im, orders_x, orders_y, NX, NY)
        operand = source_operand(factor, thin_re, thin_im, orders_x, orders_y, shift, DEPTH)
        left = row_table(orders_x, rows_x, NX)
        right = column_table(orders_y, cols_y, NY)
        return (total + weight * source_image(operand, left, right), None)
    total, _ = lax.scan(add_source, jnp.zeros((NX, DEPTH, NY), jnp.float32), (spectra, pupil_shift, window_offset, source_weight))
    intensity = total / jnp.sum(source_weight)
    fading = jnp.exp(-ABSORB * jnp.arange(DEPTH, dtype=jnp.float32))[None, :, None]
    acid_start = 1.0 - jnp.exp(-intensity * fading)
    stacked = jnp.stack([acid_start, quench_start], axis=1)
    inhibit = jnp.ones_like(acid_start)
    for step in range(STEPS):
        beside_all = jnp.roll(stacked, 1, 0) + jnp.roll(stacked, -1, 0) + jnp.roll(stacked, 1, 3) + jnp.roll(stacked, -1, 3)
        inhibit = inhibit * jnp.exp(-DEPROTECT * stacked[:, 0])
        stacked = evolve(stacked, beside_all)
    return (stacked[:, 0], stacked[:, 1], inhibit)
```

```python
import functools
import math

import jax
import jax.numpy as jnp
import numpy as np
from jax import lax
from jax.experimental import pallas as pl
from jax.experimental.pallas import tpu as pltpu
from jax.sharding import PartitionSpec as P

RADIUS = 124
CELL = 4
STEPS = 8
NX = 512
NY = 512
WIN = 256
DEPTH = 16
N_SRC, N_TX, N_TY = 8, 8, 4
ROWS, COLS = 8, 128
CELLS = 128

TWO_PI = 2.0 * math.pi
NUM_AP = 0.33
DZ_WAVE = 0.148
ABSORB = 0.05

HALF = math.pi * DZ_WAVE * (1.0 - math.sqrt(1.0 - NUM_AP * NUM_AP))
REACH = HALF * 7.5
TERMS = 5
PLANES = 8
MESH = pl.DeviceIdType.MESH


def fit(function, powers, reach):
    nodes = np.cos((2 * np.arange(400) + 1) * np.pi / 800)
    basis = np.stack([nodes**k for k in powers], 1)
    sides = np.linalg.lstsq(basis, function(reach * nodes), rcond=None)[0]
    return [float(v) for v in sides]


EVEN = fit(np.cos, (0, 2, 4), REACH)
ODD = fit(np.sin, (1, 3), REACH)
SCALE = [EVEN[0], ODD[0], -EVEN[1], -ODD[1], EVEN[2]]
PHASE_COS = fit(np.cos, (0, 2, 4, 6), 8.0 * HALF)
PHASE_SIN = fit(np.sin, (1, 3, 5), 8.0 * HALF)


def wave_tables():
    u = np.arange(WIN)
    left = np.zeros((N_TX, 2 * N_SRC * ROWS, 2 * WIN))
    for tx in range(N_TX):
        local = np.arange(N_SRC * ROWS)
        x = (local // ROWS * N_TX + tx) * ROWS + local % ROWS
        angle = TWO_PI / NX * ((x[:, None] * (u[None, :] - WIN // 2)) % NX)
        c, s = np.cos(angle), np.sin(angle)
        left[tx] = np.block([[c, -s], [s, c]])
    right = np.zeros((N_TY, 2 * WIN, 2 * COLS))
    for ty in range(N_TY):
        y = ty * COLS + np.arange(COLS)
        angle = TWO_PI / NY * ((y[None, :] * (u[:, None] - WIN // 2)) % NY)
        c, s = np.cos(angle), np.sin(angle)
        right[ty] = np.block([[c, s], [-s, c]])
    return left, right


def cell_tables():
    a = np.arange(CELLS)
    angle = TWO_PI / CELLS * ((a[:, None] * a[None, :]) % CELLS)
    c, s = np.cos(angle), np.sin(angle)
    by_column = np.block([[c, -s], [s, c]])
    by_row = np.block([[c, s], [-s, c]])
    orders = np.arange(NX) - NX // 2
    phase = TWO_PI / NX * ((orders[:, None] * np.arange(CELL)[None, :]) % NX)
    shape_re = np.cos(phase).sum(1) / NX
    shape_im = -np.sin(phase).sum(1) / NX
    shape = np.stack([shape_re, shape_im])
    shape_x = np.broadcast_to(shape[:, :, None], (2, NX, 128))
    shape_y = np.broadcast_to(shape[:, None, :], (2, 8, NY))
    return (
        by_column.astype(np.float32),
        by_row.astype(np.float32),
        shape_x.astype(np.float32),
        shape_y.astype(np.float32),
    )


def exact(left, right):
    return jnp.dot(
        left, right, precision=lax.Precision.HIGHEST, preferred_element_type=jnp.float32
    )


def image_kernel(
    shift_ref,
    offset_ref,
    levels_ref,
    weight_ref,
    all_weights_ref,
    codes_ref,
    by_column_ref,
    by_row_ref,
    shape_x_ref,
    shape_y_ref,
    spectra_ref,
    left_hbm,
    right_hbm,
    out_ref,
    left_ref,
    right_ref,
    cells_ref,
    operand_ref,
    half_ref,
    wave_ref,
    acc_ref,
    sems,
):
    j = pl.program_id(0)
    count = pl.num_programs(0)
    tables = (
        pltpu.make_async_copy(left_hbm.at[lax.axis_index("tx")], left_ref, sems.at[0]),
        pltpu.make_async_copy(right_hbm.at[lax.axis_index("ty")], right_ref, sems.at[1]),
    )

    @pl.when(j == 0)
    def _():
        for copy in tables:
            copy.start()
        codes = codes_ref[...]
        parts = []
        for part in range(2):
            grid = jnp.full(codes.shape, levels_ref[part, 3], jnp.float32)
            for level in range(3):
                grid = jnp.where(codes == level, levels_ref[part, level], grid)
            parts.append(grid)
        across = exact(jnp.concatenate(parts, axis=1), by_column_ref[...])
        both = jnp.concatenate([across[:, :CELLS], across[:, CELLS:]], axis=0)
        full = exact(by_row_ref[...], both)
        for part in range(2):
            piece = full[part * CELLS : (part + 1) * CELLS]
            cells_ref[part, 0:CELLS] = piece
            cells_ref[part, CELLS : 2 * CELLS] = piece
        acc_ref[...] = jnp.zeros_like(acc_ref)
        for copy in tables:
            copy.wait()

    first_x = offset_ref[j, 0] - shift_ref[j, 0] - WIN // 2
    first_y = offset_ref[j, 1] - shift_ref[j, 1] - WIN // 2
    start_x = first_x + NX // 2
    start_y = first_y + NY // 2
    cell_x = lax.rem(start_x, CELLS)
    roll_y = lax.rem(2 * CELLS - lax.rem(start_y, CELLS), CELLS)
    shape_y = [
        pltpu.roll(shape_y_ref[part], NY - start_y, 1)[:, :WIN] for part in range(2)
    ]
    y_re = jnp.concatenate([shape_y[0]] * 2, axis=0)
    y_im = jnp.concatenate([shape_y[1]] * 2, axis=0)
    freq_y = (
        lax.broadcasted_iota(jnp.int32, (16, WIN), 1) - WIN // 2 + offset_ref[j, 1]
    ).astype(jnp.float32)
    square_y = freq_y * freq_y
    row_in = lax.broadcasted_iota(jnp.int32, (16, WIN), 0) - WIN // 2 + offset_ref[j, 0]

    def build(step):
        at = pl.multiple_of(step * 16, 16)
        cell_at = lax.rem(cell_x + at, CELLS)
        g_re = pltpu.roll(cells_ref[0, pl.ds(cell_at, 16), :], roll_y, 1)
        g_im = pltpu.roll(cells_ref[1, pl.ds(cell_at, 16), :], roll_y, 1)
        x_re = shape_x_ref[0, pl.ds(start_x + at, 16), :]
        x_im = shape_x_ref[1, pl.ds(start_x + at, 16), :]
        gx_re = g_re * x_re - g_im * x_im
        gx_im = g_re * x_im + g_im * x_re
        gx_re = jnp.concatenate([gx_re, gx_re], axis=1)
        gx_im = jnp.concatenate([gx_im, gx_im], axis=1)
        thin_re = gx_re * y_re - gx_im * y_im
        thin_im = gx_re * y_im + gx_im * y_re
        freq_x = (row_in + at).astype(jnp.float32)
        radial = freq_x * freq_x + square_y
        limit = float(RADIUS * RADIUS)
        inside = radial <= limit
        axial = jnp.sqrt(1.0 - (NUM_AP / RADIUS) ** 2 * jnp.minimum(radial, limit))
        slope = TWO_PI * DZ_WAVE / HALF
        w = slope * (axial - 1.0) + 1.0
        square = w * w
        turn_re = jnp.full_like(w, PHASE_COS[-1])
        for value in PHASE_COS[-2::-1]:
            turn_re = turn_re * square + value
        turn_im = jnp.full_like(w, PHASE_SIN[-1])
        for value in PHASE_SIN[-2::-1]:
            turn_im = turn_im * square + value
        turn_im = turn_im * w
        zero = jnp.zeros_like(w)
        h_re = jnp.where(inside, thin_re * turn_re - thin_im * turn_im, zero)
        h_im = jnp.where(inside, thin_re * turn_im + thin_im * turn_re, zero)
        for c in range(3):
            f_re = spectra_ref[0, c, 0, pl.ds(at, 16), :].astype(jnp.float32)
            f_im = spectra_ref[0, c, 1, pl.ds(at, 16), :].astype(jnp.float32)
            s_re = f_re * h_re - f_im * h_im
            s_im = f_re * h_im + f_im * h_re
            for n in range(TERMS):
                where = slice((c * TERMS + n) * WIN, (c * TERMS + n + 1) * WIN)
                operand_ref[pl.ds(at, 16), where] = s_re.astype(jnp.bfloat16)
                operand_ref[pl.ds(WIN + at, 16), where] = s_im.astype(jnp.bfloat16)
                if n < TERMS - 1:
                    s_re = s_re * w
                    s_im = s_im * w

    @pl.loop(0, WIN // 16, unroll=2)
    def _(step):
        build(step)

    for block in range(3 * TERMS):
        halves = jnp.dot(
            left_ref[...],
            operand_ref[:, block * WIN : (block + 1) * WIN],
            preferred_element_type=jnp.float32,
        ).astype(jnp.bfloat16)
        half_ref[block * 64 : (block + 1) * 64, 0:WIN] = halves[0:64]
        half_ref[block * 64 : (block + 1) * 64, WIN : 2 * WIN] = halves[64:128]
    for c in range(3):
        span = slice(c * TERMS * 64, (c + 1) * TERMS * 64)
        wave_ref[span, :] = jnp.dot(
            half_ref[span, :], right_ref[...], preferred_element_type=jnp.float32
        )
    weight = weight_ref[lax.axis_index("src") * count + j]
    for p in range(N_SRC):
        totals = [None] * 9

        def gather(n, value):
            totals[n] = value if totals[n] is None else totals[n] + value

        for c in range(3):
            re, im = [], []
            for n in range(TERMS):
                base = (c * TERMS + n) * 64 + p * ROWS
                re.append(wave_ref[base : base + ROWS, 0:COLS] * SCALE[n])
                im.append(wave_ref[base : base + ROWS, COLS : 2 * COLS] * SCALE[n])

            def real(a, b):
                return re[a] * re[b] + im[a] * im[b]

            def imag(a, b):
                return im[a] * re[b] - re[a] * im[b]

            gather(0, real(0, 0))
            gather(1, -2.0 * imag(1, 0))
            gather(2, real(1, 1) - 2.0 * real(0, 2))
            gather(3, 2.0 * (imag(1, 2) + imag(3, 0)))
            gather(4, real(2, 2) + 2.0 * (real(0, 4) - real(1, 3)))
            gather(5, -2.0 * (imag(1, 4) + imag(3, 2)))
            gather(6, real(3, 3) - 2.0 * real(2, 4))
            gather(7, 2.0 * imag(3, 4))
            gather(8, real(4, 4))
        for n in range(9):
            acc_ref[n, p * ROWS : (p + 1) * ROWS] += weight * totals[n]

    @pl.when(j == count - 1)
    def _():
        norm = 1.0 / jnp.sum(all_weights_ref[...], axis=1, keepdims=True)
        for p in range(N_SRC):
            rows = slice(p * ROWS, (p + 1) * ROWS)
            planes = [acc_ref[n, rows] * norm for n in range(9)]
            top = planes[8]
            planes[0] = planes[0] - top * (1.0 / 128.0)
            planes[2] = planes[2] + top * 0.25
            planes[4] = planes[4] - top * 1.25
            planes[6] = planes[6] + top * 2.0
            out_ref[p] = jnp.concatenate(planes[:8], axis=0).astype(jnp.bfloat16)


def image_planes(spectra, shift, offset, weights, codes, levels):
    left, right = wave_tables()
    by_column, by_row, shape_x, shape_y = cell_tables()
    vmem = pl.BlockSpec(memory_space=pltpu.VMEM)
    smem = pl.BlockSpec(memory_space=pltpu.SMEM)
    hbm = pl.BlockSpec(memory_space=pl.ANY)
    count = spectra.shape[0]
    return pl.pallas_call(
        image_kernel,
        grid=(count,),
        out_shape=jax.ShapeDtypeStruct((N_SRC, PLANES * ROWS, COLS), jnp.bfloat16),
        in_specs=[
            smem,
            smem,
            smem,
            smem,
            vmem,
            vmem,
            vmem,
            vmem,
            vmem,
            vmem,
            pl.BlockSpec((1, 3, 2, WIN, WIN), lambda j: (j, 0, 0, 0, 0)),
            hbm,
            hbm,
        ],
        out_specs=vmem,
        scratch_shapes=[
            pltpu.VMEM((128, 2 * WIN), jnp.bfloat16),
            pltpu.VMEM((2 * WIN, 2 * COLS), jnp.bfloat16),
            pltpu.VMEM((2, 2 * CELLS, CELLS), jnp.float32),
            pltpu.VMEM((2 * WIN, 3 * TERMS * WIN), jnp.bfloat16),
            pltpu.VMEM((3 * TERMS * 64, 2 * WIN), jnp.bfloat16),
            pltpu.VMEM((3 * TERMS * 64, 2 * COLS), jnp.float32),
            pltpu.VMEM((9, 64, COLS), jnp.float32),
            pltpu.SemaphoreType.DMA((2,)),
        ],
        compiler_params=pltpu.CompilerParams(vmem_limit_bytes=48 << 20),
        name="image",
    )(
        shift,
        offset,
        levels,
        weights,
        weights.reshape(1, -1),
        codes,
        jnp.asarray(by_column),
        jnp.asarray(by_row),
        jnp.asarray(shape_x),
        jnp.asarray(shape_y),
        spectra,
        jnp.asarray(left, jnp.bfloat16),
        jnp.asarray(right, jnp.bfloat16),
    )


AROUND = [(dr, dc) for dr in (-1, 0, 1) for dc in (-1, 0, 1) if (dr, dc) != (0, 0)]


def bake_kernel(
    planes_ref,
    quench_ref,
    acid_out,
    quench_out,
    inhibit_out,
    arrived,
    own_planes,
    own_strip,
    own_quench_strip,
    near_planes,
    near_strips,
    near_quench,
    near_quench_strips,
    field,
    send_sems,
    recv_sems,
    near_send,
    near_recv,
    quench_send,
    quench_recv,
):
    src, tx, ty = lax.axis_index("src"), lax.axis_index("tx"), lax.axis_index("ty")
    place = src * N_TX + tx

    def device_at(dr, dc):
        row = lax.rem(place + dr + N_SRC * N_TX, N_SRC * N_TX)
        column = lax.rem(ty + dc + N_TY, N_TY)
        return (row // N_TX, lax.rem(row, N_TX), column)

    peers = [(lax.rem(src + d, N_SRC), tx, ty) for d in range(1, N_SRC)]
    around = [device_at(dr, dc) for dr, dc in AROUND]
    barrier = pltpu.get_barrier_semaphore()
    for device in peers + around:
        pl.semaphore_signal(barrier, inc=1, device_id=device, device_id_type=MESH)
    pl.semaphore_wait(barrier, len(peers) + len(around))

    exchange = []
    for d in range(1, N_SRC):
        copy = pltpu.make_async_remote_copy(
            src_ref=planes_ref.at[lax.rem(src + d, N_SRC)],
            dst_ref=arrived.at[d - 1],
            send_sem=send_sems.at[d - 1],
            recv_sem=recv_sems.at[d - 1],
            device_id=peers[d - 1],
            device_id_type=MESH,
        )
        copy.start()
        exchange.append(copy)

    lane = lax.broadcasted_iota(jnp.int32, (8, COLS), 1)
    group = lane // 16

    def packed(tiles):
        total = jnp.zeros((8, COLS), jnp.float32)
        for n, tile in enumerate(tiles):
            moved = pltpu.roll(tile, (8 + 16 * n) % COLS, 1)
            total = jnp.where(group == n, moved, total)
        return total

    def unpacked(merged, n):
        tile = pltpu.roll(merged, (COLS - 8 - 16 * n) % COLS, 1)
        return jnp.where((lane < 8) | (lane >= COLS - 8), tile, 0.0)

    first_half = lax.rem(lane, 16) < 8

    for k in range(2):
        own_quench_strip[k] = packed(
            [quench_ref[r, zh * 8 : zh * 8 + 8, :] for r in range(4 * k, 4 * k + 4) for zh in range(2)]
        )

    def send_around(whole, strip, near_whole, near_strip, sends, recvs):
        copies = []
        for i, (dr, dc) in enumerate(AROUND):
            if dc == 0:
                source, target = whole, near_whole.at[0 if dr == 1 else 1]
            else:
                slot = (1 - dr) * 2 + (0 if dc == 1 else 1)
                source, target = strip, near_strip.at[slot]
            copy = pltpu.make_async_remote_copy(
                src_ref=source,
                dst_ref=target,
                send_sem=sends.at[i],
                recv_sem=recvs.at[i],
                device_id=around[i],
                device_id_type=MESH,
            )
            copy.start()
            copies.append(copy)
        return copies

    quench_copies = send_around(
        quench_ref, own_quench_strip, near_quench, near_quench_strips, quench_send, quench_recv
    )

    total = planes_ref[src].astype(jnp.float32)
    for d in range(1, N_SRC):
        exchange[d - 1].wait_recv()
        total = total + arrived[d - 1].astype(jnp.float32)
    own_planes[...] = total
    own_strip[...] = packed([own_planes[n * 8 : n * 8 + 8, :] for n in range(PLANES)])
    plane_copies = send_around(
        own_planes, own_strip, near_planes, near_strips, near_send, near_recv
    )

    for copy in quench_copies:
        copy.wait_recv()
    for g in range(3):
        source = quench_ref if g == 1 else near_quench.at[0 if g == 0 else 1]
        for r in range(8):
            field[0, 1, g * 8 + r, :, 0:COLS] = source[r]
        for k in range(2):
            merged = jnp.where(
                first_half, near_quench_strips[2 * g, k], near_quench_strips[2 * g + 1, k]
            )
            for n in range(8):
                row, zh = 4 * k + n // 2, n % 2
                field[0, 1, g * 8 + row, zh * 8 : zh * 8 + 8, COLS : 2 * COLS] = unpacked(
                    merged, n
                )

    z_at = lax.broadcasted_iota(jnp.int32, (DEPTH, COLS), 0).astype(jnp.float32)
    tau = (z_at - 7.5) * (1.0 / 7.5)
    fading = jnp.exp(-ABSORB * z_at)

    def start_acid(g, get, side):
        for r in range(8):
            value = jnp.broadcast_to(get(PLANES - 1)[r : r + 1], (DEPTH, COLS))
            for n in range(PLANES - 2, -1, -1):
                value = value * tau + get(n)[r : r + 1]
            acid = 1.0 - jnp.exp(-value * fading)
            field[0, 0, g * 8 + r, :, side * COLS : (side + 1) * COLS] = acid

    start_acid(1, lambda n: own_planes[n * 8 : n * 8 + 8, :], 0)
    for copy in plane_copies:
        copy.wait_recv()
    for g in range(3):
        if g != 1:
            start_acid(g, lambda n: near_planes[0 if g == 0 else 1, n * 8 : n * 8 + 8, :], 0)
        merged = jnp.where(first_half, near_strips[2 * g], near_strips[2 * g + 1])
        tiles = [unpacked(merged, n) for n in range(PLANES)]
        start_acid(g, lambda n: tiles[n], 1)

    z_index = lax.broadcasted_iota(jnp.int32, (DEPTH, 2 * COLS), 0)

    def around_sum(slot, which, row):
        here = field[slot, which, row]
        beside = (
            field[slot, which, row - 1]
            + field[slot, which, row + 1]
            + pltpu.roll(here, 1, 1)
            + pltpu.roll(here, 2 * COLS - 1, 1)
        )
        above = jnp.where(z_index == 0, here, pltpu.roll(here, 1, 0))
        below = jnp.where(z_index == DEPTH - 1, here, pltpu.roll(here, DEPTH - 1, 0))
        return here, beside, above + below

    spent = [jnp.zeros((DEPTH, COLS), jnp.float32) for _ in range(ROWS)]
    for step in range(STEPS):
        old, new = step % 2, 1 - step % 2
        last = step == STEPS - 1
        for row in range(step + 1, 23 - step):
            a, a_beside, a_depth = around_sum(old, 0, row)
            q, q_beside, q_depth = around_sum(old, 1, row)
            reaction = 0.08 * a * q
            a_new = 0.1 * a + 0.2 * a_beside + 0.05 * a_depth - reaction
            q_new = 0.73 * q + 0.06 * q_beside + 0.015 * q_depth - reaction
            own = row - 8
            if 0 <= own < ROWS:
                spent[own] = spent[own] + a[:, :COLS]
            if last:
                acid_out[own] = a_new[:, :COLS]
                quench_out[own] = q_new[:, :COLS]
                inhibit_out[own] = jnp.exp(-0.25 * spent[own])
            else:
                field[new, 0, row] = a_new
                field[new, 1, row] = q_new

    for copy in exchange + quench_copies + plane_copies:
        copy.wait_send()


def baked(planes, quench):
    vmem = pl.BlockSpec(memory_space=pltpu.VMEM)
    tile = jax.ShapeDtypeStruct((ROWS, DEPTH, COLS), jnp.float32)
    dma = pltpu.SemaphoreType.DMA
    return pl.pallas_call(
        bake_kernel,
        out_shape=(tile, tile, tile),
        in_specs=[vmem, vmem],
        out_specs=(vmem, vmem, vmem),
        scratch_shapes=[
            pltpu.VMEM((N_SRC - 1, PLANES * ROWS, COLS), jnp.bfloat16),
            pltpu.VMEM((PLANES * ROWS, COLS), jnp.float32),
            pltpu.VMEM((8, COLS), jnp.float32),
            pltpu.VMEM((2, 8, COLS), jnp.float32),
            pltpu.VMEM((2, PLANES * ROWS, COLS), jnp.float32),
            pltpu.VMEM((6, 8, COLS), jnp.float32),
            pltpu.VMEM((2, ROWS, DEPTH, COLS), jnp.float32),
            pltpu.VMEM((6, 2, 8, COLS), jnp.float32),
            pltpu.VMEM((2, 2, 24, DEPTH, 2 * COLS), jnp.float32),
            dma((7,)),
            dma((7,)),
            dma((8,)),
            dma((8,)),
            dma((8,)),
            dma((8,)),
        ],
        compiler_params=pltpu.CompilerParams(
            collective_id=0, has_side_effects=True, vmem_limit_bytes=48 << 20
        ),
        name="bake",
    )(planes, quench)


def per_device(
    spectra, pupil_shift, window_offset, source_weight, mask_codes, levels, quench_start
):
    planes = image_planes(
        spectra, pupil_shift, window_offset, source_weight, mask_codes, levels
    )
    return baked(planes, quench_start)


def solution(mesh):
    in_specs = (
        P("src", None, None, None, None),
        P("src", None),
        P("src", None),
        P(),
        P(),
        P(),
        P(("src", "tx"), None, "ty"),
    )
    out_specs = (
        P(("src", "tx"), None, "ty"),
        P(("src", "tx"), None, "ty"),
        P(("src", "tx"), None, "ty"),
    )
    return jax.shard_map(
        per_device, mesh=mesh, in_specs=in_specs, out_specs=out_specs, check_vma=False
    )
```

```python
import functools
import math

import jax
import jax.numpy as jnp
import numpy as np
from jax import lax
from jax.experimental import pallas as pl
from jax.experimental.pallas import tpu as pltpu
from jax.sharding import PartitionSpec as P

RADIUS = 124
CELL = 4
STEPS = 8
NX = 512
NY = 512
WIN = 256
DEPTH = 16
N_SRC, N_TX, N_TY = 8, 8, 4
ROWS, COLS = 8, 128
CELLS = 128

TWO_PI = 2.0 * math.pi
NUM_AP = 0.33
DZ_WAVE = 0.148
ABSORB = 0.05

HALF = math.pi * DZ_WAVE * (1.0 - math.sqrt(1.0 - NUM_AP * NUM_AP))
REACH = HALF * 7.5
TERMS = 5
BLOCKS = 16
REACH_OFF = 3
PLANES = 8
MESH = pl.DeviceIdType.MESH


def fit(function, powers, reach):
    nodes = np.cos((2 * np.arange(400) + 1) * np.pi / 800)
    basis = np.stack([nodes**k for k in powers], 1)
    sides = np.linalg.lstsq(basis, function(reach * nodes), rcond=None)[0]
    return [float(v) for v in sides]


EVEN = fit(np.cos, (0, 2, 4), REACH)
ODD = fit(np.sin, (1, 3), REACH)
SCALE = [EVEN[0], ODD[0], -EVEN[1], -ODD[1], EVEN[2]]


def wave_tables():
    u = np.arange(WIN)
    left = np.zeros((N_TX, 2, N_SRC * ROWS, WIN))
    for tx in range(N_TX):
        local = np.arange(N_SRC * ROWS)
        x = (local // ROWS * N_TX + tx) * ROWS + local % ROWS
        angle = TWO_PI / NX * ((x[:, None] * (u[None, :] - WIN // 2)) % NX)
        c, s = np.cos(angle), np.sin(angle)
        left[tx] = np.stack([c, s])
    right = np.zeros((N_TY, 2, WIN, COLS))
    for ty in range(N_TY):
        y = ty * COLS + np.arange(COLS)
        angle = TWO_PI / NY * ((y[None, :] * (u[:, None] - WIN // 2)) % NY)
        c, s = np.cos(angle), np.sin(angle)
        right[ty] = np.stack([c, s])
    return left, right


def turn_tables():
    fx = np.arange(WIN + 8) - WIN // 2 - REACH_OFF
    fy = np.arange(WIN + 128) - WIN // 2 - REACH_OFF
    radial = fx[:, None] ** 2 + fy[None, :] ** 2
    limit = RADIUS * RADIUS
    axial = np.sqrt(1.0 - (NUM_AP / RADIUS) ** 2 * np.minimum(radial, limit))
    w = TWO_PI * DZ_WAVE * (axial - 1.0) / HALF + 1.0
    inside = radial <= limit
    turn = 8.0 * HALF * w
    table = np.stack([w, np.cos(turn) * inside, np.sin(turn) * inside])
    return np.stack(np.split(table, 3, axis=2), 1).astype(np.float32)


def cell_tables():
    a = np.arange(CELLS)
    angle = TWO_PI / CELLS * ((a[:, None] * a[None, :]) % CELLS)
    c, s = np.cos(angle), np.sin(angle)
    cell_waves = np.stack([c, s])
    orders = np.arange(NX) - NX // 2
    phase = TWO_PI / NX * ((orders[:, None] * np.arange(CELL)[None, :]) % NX)
    shape_re = np.cos(phase).sum(1) / NX
    shape_im = -np.sin(phase).sum(1) / NX
    shape = np.stack([shape_re, shape_im])
    shape_x = np.broadcast_to(shape[:, :, None], (2, NX, 128))
    shape_y = np.broadcast_to(shape[:, None, :], (2, 8, NY))
    return (
        cell_waves.astype(np.float32),
        shape_x.astype(np.float32),
        shape_y.astype(np.float32),
    )


def exact(left, right):
    return jnp.dot(
        left, right, precision=lax.Precision.HIGHEST, preferred_element_type=jnp.float32
    )


AROUND = [(dr, dc) for dr in (-1, 0, 1) for dc in (-1, 0, 1) if (dr, dc) != (0, 0)]


def image_kernel(
    shift_hbm,
    offset_hbm,
    weight_hbm,
    levels_hbm,
    codes_hbm,
    cell_waves_hbm,
    shape_x_hbm,
    shape_y_hbm,
    turn_hbm,
    left_hbm,
    right_hbm,
    spectra_hbm,
    quench_hbm,
    field,
    shift_ref,
    offset_ref,
    weight_ref,
    levels_ref,
    codes_ref,
    cell_waves_ref,
    shape_x_ref,
    shape_y_ref,
    turn_ref,
    left_in,
    right_in,
    left_ref,
    right_ref,
    spectra_ref,
    quench_ref,
    cells_ref,
    operand_a,
    operand_b,
    half_ref,
    wave_ref,
    acc_ref,
    planes_ref,
    arrived,
    own_planes,
    own_strip,
    own_quench_strip,
    near_planes,
    near_strips,
    near_quench,
    near_quench_strips,
    load_sems,
    spectra_sems,
    send_sems,
    recv_sems,
    near_send,
    near_recv,
    quench_send,
    quench_recv,
):
    src, tx, ty = lax.axis_index("src"), lax.axis_index("tx"), lax.axis_index("ty")
    place = src * N_TX + tx

    def device_at(dr, dc):
        row = lax.rem(place + dr + N_SRC * N_TX, N_SRC * N_TX)
        column = lax.rem(ty + dc + N_TY, N_TY)
        return (row // N_TX, lax.rem(row, N_TX), column)

    peers = [(lax.rem(src + d, N_SRC), tx, ty) for d in range(1, N_SRC)]
    around = [device_at(dr, dc) for dr, dc in AROUND]

    loads = {}
    pairs = [
        ("codes", codes_hbm, codes_ref),
        ("levels", levels_hbm, levels_ref),
        ("cell", cell_waves_hbm, cell_waves_ref),
        ("shift", shift_hbm, shift_ref),
        ("offset", offset_hbm, offset_ref),
        ("weight", weight_hbm, weight_ref),
        ("shape_x", shape_x_hbm, shape_x_ref),
        ("shape_y", shape_y_hbm, shape_y_ref),
        ("turn", turn_hbm, turn_ref),
        ("left", left_hbm.at[tx], left_in),
        ("right", right_hbm.at[ty], right_in),
        ("quench", quench_hbm, quench_ref),
    ]
    count = spectra_hbm.shape[0]
    spectra_loads = [
        pltpu.make_async_copy(spectra_hbm.at[j], spectra_ref.at[j], spectra_sems.at[j])
        for j in range(count)
    ]
    for i, (name, source, target) in enumerate(pairs):
        loads[name] = pltpu.make_async_copy(source, target, load_sems.at[i])
        loads[name].start()
        if name == "turn":
            spectra_loads[0].start()
    for copy in spectra_loads[1:]:
        copy.start()

    barrier = pltpu.get_barrier_semaphore()
    for device in peers + around:
        pl.semaphore_signal(barrier, inc=1, device_id=device, device_id_type=MESH)

    for name in ("codes", "levels", "cell"):
        loads[name].wait()
    codes = codes_ref[...]
    parts = []
    for part in range(2):
        grid = jnp.full(codes.shape, levels_ref[part, 3], jnp.float32)
        for level in range(3):
            grid = jnp.where(codes == level, levels_ref[part, level], grid)
        parts.append(grid)
    c, s = cell_waves_ref[0], cell_waves_ref[1]
    by_column = jnp.concatenate(
        [jnp.concatenate([c, -s], axis=1), jnp.concatenate([s, c], axis=1)], axis=0
    )
    by_row = jnp.concatenate(
        [jnp.concatenate([c, s], axis=1), jnp.concatenate([-s, c], axis=1)], axis=0
    )
    across = exact(jnp.concatenate(parts, axis=1), by_column)
    both = jnp.concatenate([across[:, :CELLS], across[:, CELLS:]], axis=0)
    full = exact(by_row, both)
    for part in range(2):
        piece = full[part * CELLS : (part + 1) * CELLS]
        cells_ref[part, 0:CELLS] = piece
        cells_ref[part, CELLS : 2 * CELLS] = piece
    operand_a[BLOCKS - 1] = jnp.zeros((2 * WIN, WIN), jnp.bfloat16)
    operand_b[BLOCKS - 1] = jnp.zeros((2 * WIN, WIN), jnp.bfloat16)
    half_ref[...] = jnp.zeros_like(half_ref)
    for name in ("shift", "offset", "weight", "shape_x", "shape_y", "turn", "left", "right"):
        loads[name].wait()

    rows = N_SRC * ROWS
    left_ref[0:rows, 0:WIN] = left_in[0]
    left_ref[0:rows, WIN : 2 * WIN] = -left_in[1]
    left_ref[rows : 2 * rows, 0:WIN] = left_in[1]
    left_ref[rows : 2 * rows, WIN : 2 * WIN] = left_in[0]
    right_ref[0:WIN, 0:COLS] = right_in[0]
    right_ref[0:WIN, COLS : 2 * COLS] = right_in[1]
    right_ref[WIN : 2 * WIN, 0:COLS] = -right_in[1]
    right_ref[WIN : 2 * WIN, COLS : 2 * COLS] = right_in[0]

    total_weight = weight_ref[0]
    for k in range(1, weight_ref.shape[0]):
        total_weight = total_weight + weight_ref[k]
    norm = 1.0 / jnp.full((1, COLS), total_weight, jnp.float32)

    def builder(j, operand):
        spectra_loads[j].wait()
        off_x, off_y = offset_ref[0, j], offset_ref[1, j]
        start_x = off_x - shift_ref[0, j] - WIN // 2 + NX // 2
        start_y = off_y - shift_ref[1, j] - WIN // 2 + NY // 2
        cell_x = lax.rem(start_x, CELLS)
        roll_y = lax.rem(2 * CELLS - lax.rem(start_y, CELLS), CELLS)
        turn_x = off_x + REACH_OFF
        turn_y = lax.rem(WIN + 128 - (off_y + REACH_OFF), WIN + 128)
        shape_y = [
            pltpu.roll(shape_y_ref[part], NY - start_y, 1)[:, :WIN] for part in range(2)
        ]
        y_re = jnp.concatenate([shape_y[0]] * 2, axis=0)
        y_im = jnp.concatenate([shape_y[1]] * 2, axis=0)

        def build(step):
            at = pl.multiple_of(step * 16, 16)
            cell_at = lax.rem(cell_x + at, CELLS)
            g_re = pltpu.roll(cells_ref[0, pl.ds(cell_at, 16), :], roll_y, 1)
            g_im = pltpu.roll(cells_ref[1, pl.ds(cell_at, 16), :], roll_y, 1)
            x_re = shape_x_ref[0, pl.ds(start_x + at, 16), :]
            x_im = shape_x_ref[1, pl.ds(start_x + at, 16), :]
            gx_re = g_re * x_re - g_im * x_im
            gx_im = g_re * x_im + g_im * x_re
            gx_re = jnp.concatenate([gx_re, gx_re], axis=1)
            gx_im = jnp.concatenate([gx_im, gx_im], axis=1)
            thin_re = gx_re * y_re - gx_im * y_im
            thin_im = gx_re * y_im + gx_im * y_re
            w, turn_re, turn_im = (
                pltpu.roll(
                    jnp.concatenate(
                        [turn_ref[k, t, pl.ds(turn_x + at, 16), :] for t in range(3)], axis=1
                    ),
                    turn_y,
                    1,
                )[:, :WIN]
                for k in range(3)
            )
            w = w.astype(jnp.bfloat16)
            h_re = thin_re * turn_re - thin_im * turn_im
            h_im = thin_re * turn_im + thin_im * turn_re
            for c in range(3):
                f_re = spectra_ref[j, c, 0, pl.ds(at, 16), :].astype(jnp.float32)
                f_im = spectra_ref[j, c, 1, pl.ds(at, 16), :].astype(jnp.float32)
                s_re = (f_re * h_re - f_im * h_im).astype(jnp.bfloat16)
                s_im = (f_re * h_im + f_im * h_re).astype(jnp.bfloat16)
                for n in range(TERMS):
                    operand[c * TERMS + n, pl.ds(at, 16), :] = s_re
                    operand[c * TERMS + n, pl.ds(WIN + at, 16), :] = s_im
                    if n < TERMS - 1:
                        s_re = s_re * w
                        s_im = s_im * w

        return build

    def transform(quad, operand, store):
        parity = lax.rem(quad, 2)
        before = pl.multiple_of(lax.rem(quad + 3, 4) * 256, 256)
        wave_ref[pl.ds(before, 256), :] = jnp.dot(
            half_ref[1 - parity], right_ref[...], preferred_element_type=jnp.float32
        )
        for b in range(4):
            halves = jnp.dot(
                left_ref[...], operand[quad * 4 + b], preferred_element_type=jnp.float32
            ).astype(jnp.bfloat16)
            half_ref[parity, b * 64 : (b + 1) * 64, 0:WIN] = halves[0:64]
            half_ref[parity, b * 64 : (b + 1) * 64, WIN : 2 * WIN] = halves[64:128]
            if store is not None:
                store(quad * 4 + b)

    def gather(j):
        wave_ref[768:1024, :] = jnp.dot(
            half_ref[1], right_ref[...], preferred_element_type=jnp.float32
        )
        weight = weight_ref[src * count + j] * norm
        for p in range(N_SRC):
            totals = [None] * 9

            def add(n, value):
                totals[n] = value if totals[n] is None else totals[n] + value

            for c in range(3):
                re, im = [], []
                for n in range(TERMS):
                    base = (c * TERMS + n) * 64 + p * ROWS
                    re.append(wave_ref[base : base + ROWS, 0:COLS] * SCALE[n])
                    im.append(wave_ref[base : base + ROWS, COLS : 2 * COLS] * SCALE[n])

                def real(a, b):
                    return re[a] * re[b] + im[a] * im[b]

                def imag(a, b):
                    return im[a] * re[b] - re[a] * im[b]

                add(0, real(0, 0))
                add(1, -2.0 * imag(1, 0))
                add(2, real(1, 1) - 2.0 * real(0, 2))
                add(3, 2.0 * (imag(1, 2) + imag(3, 0)))
                add(4, real(2, 2) + 2.0 * (real(0, 4) - real(1, 3)))
                add(5, -2.0 * (imag(1, 4) + imag(3, 2)))
                add(6, real(3, 3) - 2.0 * real(2, 4))
                add(7, 2.0 * imag(3, 4))
                add(8, real(4, 4))
            planes = [weight * value for value in totals]
            planes[0] = planes[0] - planes[8] * (1.0 / 128.0)
            planes[2] = planes[2] + planes[8] * 0.25
            planes[4] = planes[4] - planes[8] * 1.25
            planes[6] = planes[6] + planes[8] * 2.0
            if j > 0:
                planes = [
                    planes[n] + acc_ref[p, n * ROWS : (n + 1) * ROWS, :] for n in range(PLANES)
                ]
            if j < count - 1:
                for n in range(PLANES):
                    acc_ref[p, n * ROWS : (n + 1) * ROWS, :] = planes[n]
            else:
                planes_ref[p] = jnp.concatenate(planes[:PLANES], axis=0).astype(jnp.bfloat16)

    operands = (operand_a, operand_b)
    build = builder(0, operands[0])

    @pl.loop(0, 4)
    def _(quad):
        for b in range(4):
            build(quad * 4 + b)

    for j in range(count):
        build = builder(j + 1, operands[(j + 1) % 2]) if j + 1 < count else None
        pl.loop(0, 4)(functools.partial(transform, operand=operands[j % 2], store=build))
        gather(j)

    pl.semaphore_wait(barrier, len(peers) + len(around))

    exchange = []
    for d in range(1, N_SRC):
        copy = pltpu.make_async_remote_copy(
            src_ref=planes_ref.at[lax.rem(src + d, N_SRC)],
            dst_ref=arrived.at[d - 1],
            send_sem=send_sems.at[d - 1],
            recv_sem=recv_sems.at[d - 1],
            device_id=peers[d - 1],
            device_id_type=MESH,
        )
        copy.start()
        exchange.append(copy)

    loads["quench"].wait()
    lane = lax.broadcasted_iota(jnp.int32, (8, COLS), 1)
    group = lane // 16

    def packed(tiles):
        total = jnp.zeros((8, COLS), jnp.float32)
        for n, tile in enumerate(tiles):
            moved = pltpu.roll(tile, (8 + 16 * n) % COLS, 1)
            total = jnp.where(group == n, moved, total)
        return total

    def unpacked(merged, n):
        tile = pltpu.roll(merged, (COLS - 8 - 16 * n) % COLS, 1)
        return jnp.where((lane < 8) | (lane >= COLS - 8), tile, 0.0)

    first_half = lax.rem(lane, 16) < 8

    for k in range(2):
        own_quench_strip[k] = packed(
            [quench_ref[r, zh * 8 : zh * 8 + 8, :] for r in range(4 * k, 4 * k + 4) for zh in range(2)]
        )

    def send_around(whole, strip, near_whole, near_strip, sends, recvs):
        copies = []
        for i, (dr, dc) in enumerate(AROUND):
            if dc == 0:
                source, target = whole, near_whole.at[0 if dr == 1 else 1]
            else:
                slot = (1 - dr) * 2 + (0 if dc == 1 else 1)
                source, target = strip, near_strip.at[slot]
            copy = pltpu.make_async_remote_copy(
                src_ref=source,
                dst_ref=target,
                send_sem=sends.at[i],
                recv_sem=recvs.at[i],
                device_id=around[i],
                device_id_type=MESH,
            )
            copy.start()
            copies.append(copy)
        return copies

    quench_copies = send_around(
        quench_ref, own_quench_strip, near_quench, near_quench_strips, quench_send, quench_recv
    )

    total = planes_ref[src].astype(jnp.float32)
    for d in range(1, N_SRC):
        exchange[d - 1].wait_recv()
        total = total + arrived[d - 1].astype(jnp.float32)
    own_planes[...] = total
    own_strip[...] = packed([own_planes[n * 8 : n * 8 + 8, :] for n in range(PLANES)])
    plane_copies = send_around(
        own_planes, own_strip, near_planes, near_strips, near_send, near_recv
    )

    for copy in quench_copies:
        copy.wait_recv()
    for g in range(3):
        source = quench_ref if g == 1 else near_quench.at[0 if g == 0 else 1]
        for r in range(8):
            field[1, g * 8 + r, :, 0:COLS] = source[r]
        for k in range(2):
            merged = jnp.where(
                first_half, near_quench_strips[2 * g, k], near_quench_strips[2 * g + 1, k]
            )
            for n in range(8):
                row, zh = 4 * k + n // 2, n % 2
                field[1, g * 8 + row, zh * 8 : zh * 8 + 8, COLS : 2 * COLS] = unpacked(
                    merged, n
                )

    z_at = lax.broadcasted_iota(jnp.int32, (DEPTH, COLS), 0).astype(jnp.float32)
    tau = (z_at - 7.5) * (1.0 / 7.5)
    fading = jnp.exp(-ABSORB * z_at)

    def start_acid(g, get, side):
        for r in range(8):
            value = jnp.broadcast_to(get(PLANES - 1)[r : r + 1], (DEPTH, COLS))
            for n in range(PLANES - 2, -1, -1):
                value = value * tau + get(n)[r : r + 1]
            acid = 1.0 - jnp.exp(-value * fading)
            field[0, g * 8 + r, :, side * COLS : (side + 1) * COLS] = acid

    start_acid(1, lambda n: own_planes[n * 8 : n * 8 + 8, :], 0)
    for copy in plane_copies:
        copy.wait_recv()
    for g in range(3):
        if g != 1:
            start_acid(g, lambda n: near_planes[0 if g == 0 else 1, n * 8 : n * 8 + 8, :], 0)
        merged = jnp.where(first_half, near_strips[2 * g], near_strips[2 * g + 1])
        tiles = [unpacked(merged, n) for n in range(PLANES)]
        start_acid(g, lambda n: tiles[n], 1)

    for copy in exchange + quench_copies + plane_copies:
        copy.wait_send()


def halo_field(spectra, shift, offset, weights, codes, levels, quench):
    left, right = wave_tables()
    cell_waves, shape_x, shape_y = cell_tables()
    turn = turn_tables()
    bf16, f32, dma = jnp.bfloat16, jnp.float32, pltpu.SemaphoreType.DMA
    vmem, smem = pltpu.VMEM, pltpu.SMEM
    count = spectra.shape[0]
    return pl.pallas_call(
        image_kernel,
        out_shape=jax.ShapeDtypeStruct((2, 3 * ROWS, DEPTH, 2 * COLS), f32),
        in_specs=[pl.BlockSpec(memory_space=pltpu.HBM)] * 13,
        out_specs=pl.BlockSpec(memory_space=pltpu.VMEM),
        scratch_shapes=[
            smem((2, count), jnp.int32),
            smem((2, count), jnp.int32),
            smem(weights.shape, f32),
            smem(levels.shape, f32),
            vmem(codes.shape, jnp.int32),
            vmem(cell_waves.shape, f32),
            vmem(shape_x.shape, f32),
            vmem(shape_y.shape, f32),
            vmem(turn.shape, f32),
            vmem(left.shape[1:], bf16),
            vmem(right.shape[1:], bf16),
            vmem((2 * N_SRC * ROWS, 2 * WIN), bf16),
            vmem((2 * WIN, 2 * COLS), bf16),
            vmem(spectra.shape, bf16),
            vmem(quench.shape, f32),
            vmem((2, 2 * CELLS, CELLS), f32),
            vmem((BLOCKS, 2 * WIN, WIN), bf16),
            vmem((BLOCKS, 2 * WIN, WIN), bf16),
            vmem((2, 256, 2 * WIN), bf16),
            vmem((BLOCKS * 64, 2 * COLS), f32),
            vmem((N_SRC, PLANES * ROWS, COLS), f32),
            vmem((N_SRC, PLANES * ROWS, COLS), bf16),
            vmem((N_SRC - 1, PLANES * ROWS, COLS), bf16),
            vmem((PLANES * ROWS, COLS), f32),
            vmem((8, COLS), f32),
            vmem((2, 8, COLS), f32),
            vmem((2, PLANES * ROWS, COLS), f32),
            vmem((6, 8, COLS), f32),
            vmem((2, ROWS, DEPTH, COLS), f32),
            vmem((6, 2, 8, COLS), f32),
            dma((12,)),
            dma((count,)),
            dma((7,)),
            dma((7,)),
            dma((8,)),
            dma((8,)),
            dma((8,)),
            dma((8,)),
        ],
        compiler_params=pltpu.CompilerParams(
            collective_id=0, has_side_effects=True, vmem_limit_bytes=40 << 20
        ),
        name="image",
    )(*(pltpu.with_memory_space_constraint(value, pltpu.HBM) for value in (
        shift.T,
        offset.T,
        weights,
        levels,
        codes,
        jnp.asarray(cell_waves),
        jnp.asarray(shape_x),
        jnp.asarray(shape_y),
        jnp.asarray(turn),
        jnp.asarray(left, bf16),
        jnp.asarray(right, bf16),
        spectra,
        quench,
    )))


def bake_kernel(start, acid_hbm, quench_hbm, inhibit_hbm, field, acid_out, quench_out, inhibit_out, sems):
    z_index = lax.broadcasted_iota(jnp.int32, (DEPTH, 2 * COLS), 0)

    def around_sum(held, which, row):
        here = held[which, row]
        beside = (
            held[which, row - 1]
            + held[which, row + 1]
            + pltpu.roll(here, 1, 1)
            + pltpu.roll(here, 2 * COLS - 1, 1)
        )
        above = jnp.where(z_index == 0, here, pltpu.roll(here, 1, 0))
        below = jnp.where(z_index == DEPTH - 1, here, pltpu.roll(here, DEPTH - 1, 0))
        return here, beside, above + below

    spent = [jnp.zeros((DEPTH, COLS), jnp.float32) for _ in range(ROWS)]
    for step in range(STEPS):
        old = start if step == 0 else field.at[step % 2]
        new = field.at[1 - step % 2]
        last = step == STEPS - 1
        for row in range(step + 1, 23 - step):
            a, a_beside, a_depth = around_sum(old, 0, row)
            q, q_beside, q_depth = around_sum(old, 1, row)
            reaction = 0.08 * a * q
            a_new = 0.1 * a + 0.2 * a_beside + 0.05 * a_depth - reaction
            q_new = 0.73 * q + 0.06 * q_beside + 0.015 * q_depth - reaction
            own = row - 8
            if 0 <= own < ROWS:
                spent[own] = spent[own] + a[:, :COLS]
            if last:
                acid_out[own] = a_new[:, :COLS]
                quench_out[own] = q_new[:, :COLS]
                inhibit_out[own] = jnp.exp(-0.25 * spent[own])
            else:
                new[0, row] = a_new
                new[1, row] = q_new

    copies = [
        pltpu.make_async_copy(source, target, sems.at[i])
        for i, (source, target) in enumerate(
            ((acid_out, acid_hbm), (quench_out, quench_hbm), (inhibit_out, inhibit_hbm))
        )
    ]
    for copy in copies:
        copy.start()
    for copy in copies:
        copy.wait()


def baked(start):
    tile = (ROWS, DEPTH, COLS)
    out = jax.ShapeDtypeStruct(tile, jnp.float32)
    return pl.pallas_call(
        bake_kernel,
        out_shape=(out, out, out),
        in_specs=[pl.BlockSpec(memory_space=pltpu.VMEM)],
        out_specs=(pl.BlockSpec(memory_space=pltpu.HBM),) * 3,
        scratch_shapes=[
            pltpu.VMEM((2, 2, 24, DEPTH, 2 * COLS), jnp.float32),
            pltpu.VMEM(tile, jnp.float32),
            pltpu.VMEM(tile, jnp.float32),
            pltpu.VMEM(tile, jnp.float32),
            pltpu.SemaphoreType.DMA((3,)),
        ],
        compiler_params=pltpu.CompilerParams(vmem_limit_bytes=16 << 20),
        name="bake",
    )(start)


def per_device(
    spectra, pupil_shift, window_offset, source_weight, mask_codes, levels, quench_start
):
    return baked(
        halo_field(
            spectra,
            pupil_shift,
            window_offset,
            source_weight,
            mask_codes,
            levels,
            quench_start,
        )
    )


def solution(mesh):
    in_specs = (
        P("src", None, None, None, None),
        P("src", None),
        P("src", None),
        P(),
        P(),
        P(),
        P(("src", "tx"), None, "ty"),
    )
    out_specs = (
        P(("src", "tx"), None, "ty"),
        P(("src", "tx"), None, "ty"),
        P(("src", "tx"), None, "ty"),
    )
    return jax.shard_map(
        per_device, mesh=mesh, in_specs=in_specs, out_specs=out_specs, check_vma=False
    )
```

```python
import functools
import math

import jax
import jax.numpy as jnp
import numpy as np
from jax import lax
from jax.experimental import pallas as pl
from jax.experimental.pallas import tpu as pltpu
from jax.sharding import PartitionSpec as P

RADIUS = 124
CELL = 4
STEPS = 8
NX = 512
NY = 512
WIN = 256
DEPTH = 16
N_SRC, N_TX, N_TY = 8, 8, 4
ROWS, COLS = 8, 128
CELLS = 128

TWO_PI = 2.0 * math.pi
NUM_AP = 0.33
DZ_WAVE = 0.148
ABSORB = 0.05

HALF = math.pi * DZ_WAVE * (1.0 - math.sqrt(1.0 - NUM_AP * NUM_AP))
REACH = HALF * 7.5
TERMS = 5
EARLY = 0
REACH_OFF = 3
PLANES = 8
MESH = pl.DeviceIdType.MESH


def fit(function, powers, reach):
    nodes = np.cos((2 * np.arange(400) + 1) * np.pi / 800)
    basis = np.stack([nodes**k for k in powers], 1)
    sides = np.linalg.lstsq(basis, function(reach * nodes), rcond=None)[0]
    return [float(v) for v in sides]


EVEN = fit(np.cos, (0, 2, 4), REACH)
ODD = fit(np.sin, (1, 3), REACH)
SCALE = [EVEN[0], ODD[0], -EVEN[1], -ODD[1], EVEN[2]]


def wave_tables():
    u = np.arange(WIN)
    left = np.zeros((N_TX, 2, N_SRC * ROWS, WIN))
    for tx in range(N_TX):
        local = np.arange(N_SRC * ROWS)
        x = (local // ROWS * N_TX + tx) * ROWS + local % ROWS
        angle = TWO_PI / NX * ((x[:, None] * (u[None, :] - WIN // 2)) % NX)
        c, s = np.cos(angle), np.sin(angle)
        left[tx] = np.stack([c, s])
    right = np.zeros((N_TY, 2, WIN, COLS))
    for ty in range(N_TY):
        y = ty * COLS + np.arange(COLS)
        angle = TWO_PI / NY * ((y[None, :] * (u[:, None] - WIN // 2)) % NY)
        c, s = np.cos(angle), np.sin(angle)
        right[ty] = np.stack([c, s])
    return left, right


def turn_tables():
    fx = np.arange(WIN + 8) - WIN // 2 - REACH_OFF
    fy = np.arange(WIN + 128) - WIN // 2 - REACH_OFF
    radial = fx[:, None] ** 2 + fy[None, :] ** 2
    limit = RADIUS * RADIUS
    axial = np.sqrt(1.0 - (NUM_AP / RADIUS) ** 2 * np.minimum(radial, limit))
    w = TWO_PI * DZ_WAVE * (axial - 1.0) / HALF + 1.0
    inside = radial <= limit
    turn = 8.0 * HALF * w
    table = np.stack([w, np.cos(turn) * inside, np.sin(turn) * inside])
    return np.stack(np.split(table, 3, axis=2), 1).astype(np.float32)


def cell_tables():
    a = np.arange(CELLS)
    angle = TWO_PI / CELLS * ((a[:, None] * a[None, :]) % CELLS)
    c, s = np.cos(angle), np.sin(angle)
    cell_waves = np.stack([c, s])
    orders = np.arange(NX) - NX // 2
    phase = TWO_PI / NX * ((orders[:, None] * np.arange(CELL)[None, :]) % NX)
    shape_re = np.cos(phase).sum(1) / NX
    shape_im = -np.sin(phase).sum(1) / NX
    shape = np.stack([shape_re, shape_im])
    shape_x = np.broadcast_to(shape[:, :, None], (2, NX, 128))
    shape_y = np.broadcast_to(shape[:, None, :], (2, 8, NY))
    return (
        cell_waves.astype(np.float32),
        shape_x.astype(np.float32),
        shape_y.astype(np.float32),
    )


def exact(left, right):
    return jnp.dot(
        left, right, precision=lax.Precision.HIGHEST, preferred_element_type=jnp.float32
    )


AROUND = [(dr, dc) for dr in (-1, 0, 1) for dc in (-1, 0, 1) if (dr, dc) != (0, 0)]


def image_kernel(
    shift_hbm,
    offset_hbm,
    weight_hbm,
    levels_hbm,
    codes_hbm,
    cell_waves_hbm,
    shape_x_hbm,
    shape_y_hbm,
    turn_hbm,
    left_hbm,
    right_hbm,
    spectra_hbm,
    quench_hbm,
    field,
    shift_ref,
    offset_ref,
    weight_ref,
    levels_ref,
    codes_ref,
    cell_waves_ref,
    shape_x_ref,
    shape_y_ref,
    turn_ref,
    left_in,
    right_in,
    left_ref,
    right_ref,
    spectra_ref,
    quench_ref,
    cells_ref,
    operand_a,
    operand_b,
    half_ref,
    wave_a,
    wave_b,
    acc_ref,
    planes_ref,
    arrived,
    own_planes,
    own_strip,
    own_quench_strip,
    near_planes,
    near_strips,
    near_quench,
    near_quench_strips,
    load_sems,
    spectra_sems,
    send_sems,
    recv_sems,
    near_send,
    near_recv,
    quench_send,
    quench_recv,
):
    src, tx, ty = lax.axis_index("src"), lax.axis_index("tx"), lax.axis_index("ty")
    place = src * N_TX + tx

    def device_at(dr, dc):
        row = lax.rem(place + dr + N_SRC * N_TX, N_SRC * N_TX)
        column = lax.rem(ty + dc + N_TY, N_TY)
        return (row // N_TX, lax.rem(row, N_TX), column)

    peers = [(lax.rem(src + d, N_SRC), tx, ty) for d in range(1, N_SRC)]
    around = [device_at(dr, dc) for dr, dc in AROUND]

    loads = {}
    pairs = [
        ("codes", codes_hbm, codes_ref),
        ("levels", levels_hbm, levels_ref),
        ("cell", cell_waves_hbm, cell_waves_ref),
        ("shift", shift_hbm, shift_ref),
        ("offset", offset_hbm, offset_ref),
        ("weight", weight_hbm, weight_ref),
        ("shape_x", shape_x_hbm, shape_x_ref),
        ("shape_y", shape_y_hbm, shape_y_ref),
        ("turn", turn_hbm, turn_ref),
        ("left", left_hbm.at[tx], left_in),
        ("right", right_hbm.at[ty], right_in),
        ("quench", quench_hbm, quench_ref),
    ]
    count = spectra_hbm.shape[0]
    spectra_loads = [
        pltpu.make_async_copy(spectra_hbm.at[j], spectra_ref.at[j], spectra_sems.at[j])
        for j in range(count)
    ]
    for i, (name, source, target) in enumerate(pairs):
        loads[name] = pltpu.make_async_copy(source, target, load_sems.at[i])
        loads[name].start()
        if name == "turn":
            spectra_loads[0].start()
    for copy in spectra_loads[1:]:
        copy.start()

    barrier = pltpu.get_barrier_semaphore()
    for device in peers + around:
        pl.semaphore_signal(barrier, inc=1, device_id=device, device_id_type=MESH)

    for name in ("codes", "levels", "cell"):
        loads[name].wait()
    codes = codes_ref[...]
    parts = []
    for part in range(2):
        grid = jnp.full(codes.shape, levels_ref[part, 3], jnp.float32)
        for level in range(3):
            grid = jnp.where(codes == level, levels_ref[part, level], grid)
        parts.append(grid)
    c, s = cell_waves_ref[0], cell_waves_ref[1]
    by_column = jnp.concatenate(
        [jnp.concatenate([c, -s], axis=1), jnp.concatenate([s, c], axis=1)], axis=0
    )
    by_row = jnp.concatenate(
        [jnp.concatenate([c, s], axis=1), jnp.concatenate([-s, c], axis=1)], axis=0
    )
    across = exact(jnp.concatenate(parts, axis=1), by_column)
    both = jnp.concatenate([across[:, :CELLS], across[:, CELLS:]], axis=0)
    full = exact(by_row, both)
    for part in range(2):
        piece = full[part * CELLS : (part + 1) * CELLS]
        cells_ref[part, 0:CELLS] = piece
        cells_ref[part, CELLS : 2 * CELLS] = piece
    for name in ("shift", "offset", "weight", "shape_x", "shape_y", "turn", "left", "right"):
        loads[name].wait()

    rows = N_SRC * ROWS
    left_ref[0:rows, 0:WIN] = left_in[0]
    left_ref[0:rows, WIN : 2 * WIN] = -left_in[1]
    left_ref[rows : 2 * rows, 0:WIN] = left_in[1]
    left_ref[rows : 2 * rows, WIN : 2 * WIN] = left_in[0]
    right_ref[0:WIN, 0:COLS] = right_in[0]
    right_ref[0:WIN, COLS : 2 * COLS] = right_in[1]
    right_ref[WIN : 2 * WIN, 0:COLS] = -right_in[1]
    right_ref[WIN : 2 * WIN, COLS : 2 * COLS] = right_in[0]

    total_weight = weight_ref[0]
    for k in range(1, weight_ref.shape[0]):
        total_weight = total_weight + weight_ref[k]
    norm = 1.0 / jnp.full((1, COLS), total_weight, jnp.float32)

    def builder(j, operand):
        spectra_loads[j].wait()
        off_x, off_y = offset_ref[0, j], offset_ref[1, j]
        start_x = off_x - shift_ref[0, j] - WIN // 2 + NX // 2
        start_y = off_y - shift_ref[1, j] - WIN // 2 + NY // 2
        cell_x = lax.rem(start_x, CELLS)
        roll_y = lax.rem(2 * CELLS - lax.rem(start_y, CELLS), CELLS)
        turn_x = off_x + REACH_OFF
        turn_y = lax.rem(COLS - (off_y + REACH_OFF), COLS)
        shape_y = [
            pltpu.roll(shape_y_ref[part], NY - start_y, 1)[:, :WIN] for part in range(2)
        ]
        y_both = [jnp.concatenate([value] * 2, axis=0) for value in shape_y]

        lane = lax.broadcasted_iota(jnp.int32, (16, COLS), 1)
        kept = lane < COLS - (off_y + REACH_OFF)

        def turned(k, at):
            moved = [
                pltpu.roll(turn_ref[k, t, pl.ds(turn_x + at, 16), :], turn_y, 1)
                for t in range(3)
            ]
            return [jnp.where(kept, moved[t], moved[t + 1]) for t in range(2)]

        def build(step):
            at = step * 16 if isinstance(step, int) else pl.multiple_of(step * 16, 16)
            cell_at = lax.rem(cell_x + at, CELLS)
            g_re = pltpu.roll(cells_ref[0, pl.ds(cell_at, 16), :], roll_y, 1)
            g_im = pltpu.roll(cells_ref[1, pl.ds(cell_at, 16), :], roll_y, 1)
            x_re = shape_x_ref[0, pl.ds(start_x + at, 16), :]
            x_im = shape_x_ref[1, pl.ds(start_x + at, 16), :]
            gx_re = g_re * x_re - g_im * x_im
            gx_im = g_re * x_im + g_im * x_re
            w_both, turn_re_both, turn_im_both = (turned(k, at) for k in range(3))
            w = jnp.concatenate(w_both, axis=1).astype(jnp.bfloat16)
            turn_re = jnp.concatenate(turn_re_both, axis=1)
            turn_im = jnp.concatenate(turn_im_both, axis=1)
            gx_re = jnp.concatenate([gx_re, gx_re], axis=1)
            gx_im = jnp.concatenate([gx_im, gx_im], axis=1)
            y_re, y_im = y_both
            thin_re = gx_re * y_re - gx_im * y_im
            thin_im = gx_re * y_im + gx_im * y_re
            h_re = thin_re * turn_re - thin_im * turn_im
            h_im = thin_re * turn_im + thin_im * turn_re
            for c in range(3):
                f_re = spectra_ref[j, c, 0, pl.ds(at, 16), :].astype(jnp.float32)
                f_im = spectra_ref[j, c, 1, pl.ds(at, 16), :].astype(jnp.float32)
                s_re = (f_re * h_re - f_im * h_im).astype(jnp.bfloat16)
                s_im = (f_re * h_im + f_im * h_re).astype(jnp.bfloat16)
                for n in range(TERMS):
                    operand[c * TERMS + n, pl.ds(at, 16), :] = s_re
                    operand[c * TERMS + n, pl.ds(WIN + at, 16), :] = s_im
                    if n < TERMS - 1:
                        s_re = s_re * w
                        s_im = s_im * w

        return build

    def first(operand, block):
        halves = jnp.dot(
            left_ref[...], operand[block], preferred_element_type=jnp.float32
        ).astype(jnp.bfloat16)
        half_ref[block * 64 : (block + 1) * 64, 0:WIN] = halves[0:64]
        half_ref[block * 64 : (block + 1) * 64, WIN : 2 * WIN] = halves[64:128]

    def second(wave, c):
        span = slice(c * TERMS * 64, (c + 1) * TERMS * 64)
        wave[span, :] = jnp.dot(
            half_ref[span, :], right_ref[...], preferred_element_type=jnp.float32
        )

    def gather(j, wave, p):
        at = p * ROWS
        if j == count - 1:
            at = pl.multiple_of(at, ROWS)
        weight = weight_ref[src * count + j] * norm
        totals = [None] * 9

        def add(n, value):
            totals[n] = value if totals[n] is None else totals[n] + value

        for c in range(3):
            re, im = [], []
            for n in range(TERMS):
                rows = pl.ds((c * TERMS + n) * 64 + at, ROWS)
                re.append(wave[rows, 0:COLS] * SCALE[n])
                im.append(wave[rows, COLS : 2 * COLS] * SCALE[n])

            def real(a, b):
                return re[a] * re[b] + im[a] * im[b]

            def imag(a, b):
                return im[a] * re[b] - re[a] * im[b]

            add(0, real(0, 0))
            add(1, -2.0 * imag(1, 0))
            add(2, real(1, 1) - 2.0 * real(0, 2))
            add(3, 2.0 * (imag(1, 2) + imag(3, 0)))
            add(4, real(2, 2) + 2.0 * (real(0, 4) - real(1, 3)))
            add(5, -2.0 * (imag(1, 4) + imag(3, 2)))
            add(6, real(3, 3) - 2.0 * real(2, 4))
            add(7, 2.0 * imag(3, 4))
            add(8, real(4, 4))
        planes = [weight * value for value in totals]
        planes[0] = planes[0] - planes[8] * (1.0 / 128.0)
        planes[2] = planes[2] + planes[8] * 0.25
        planes[4] = planes[4] - planes[8] * 1.25
        planes[6] = planes[6] + planes[8] * 2.0
        if j > 0:
            planes = [
                planes[n] + acc_ref[p, n * ROWS : (n + 1) * ROWS, :] for n in range(PLANES)
            ]
        if j < count - 1:
            for n in range(PLANES):
                acc_ref[p, n * ROWS : (n + 1) * ROWS, :] = planes[n]
        else:
            planes_ref[p] = jnp.concatenate(planes[:PLANES], axis=0).astype(jnp.bfloat16)

    lane = lax.broadcasted_iota(jnp.int32, (8, COLS), 1)
    group = lane // 16

    def packed(tiles):
        total = jnp.zeros((8, COLS), jnp.float32)
        for n, tile in enumerate(tiles):
            moved = pltpu.roll(tile, (8 + 16 * n) % COLS, 1)
            total = jnp.where(group == n, moved, total)
        return total

    def unpacked(merged, n):
        tile = pltpu.roll(merged, (COLS - 8 - 16 * n) % COLS, 1)
        return jnp.where((lane < 8) | (lane >= COLS - 8), tile, 0.0)

    first_half = lax.rem(lane, 16) < 8

    def send_around(whole, strip, near_whole, near_strip, sends, recvs):
        copies = []
        for i, (dr, dc) in enumerate(AROUND):
            if dc == 0:
                source, target = whole, near_whole.at[0 if dr == 1 else 1]
            else:
                slot = (1 - dr) * 2 + (0 if dc == 1 else 1)
                source, target = strip, near_strip.at[slot]
            copy = pltpu.make_async_remote_copy(
                src_ref=source,
                dst_ref=target,
                send_sem=sends.at[i],
                recv_sem=recvs.at[i],
                device_id=around[i],
                device_id_type=MESH,
            )
            copy.start()
            copies.append(copy)
        return copies

    operands = (operand_a, operand_b)
    waves = (wave_a, wave_b)
    build = builder(0, operands[0])

    @pl.loop(0, 4)
    def _(quad):
        for b in range(4):
            build(quad * 4 + b)

    for j in range(count):
        build = builder(j + 1, operands[(j + 1) % 2]) if j + 1 < count else None
        for step in range(WIN // 16):
            if step < 3 * TERMS:
                first(operands[j % 2], step)
            if build is not None:
                build(step)
            if j > 0 and step % 2 == 0:
                gather(j - 1, waves[(j - 1) % 2], step // 2)
            if step in (5, 10, 15):
                second(waves[j % 2], step // 5 - 1)
        if j == EARLY:
            pl.semaphore_wait(barrier, len(peers) + len(around))
            loads["quench"].wait()
            for k in range(2):
                own_quench_strip[k] = packed(
                    [quench_ref[r, zh * 8 : zh * 8 + 8, :] for r in range(4 * k, 4 * k + 4) for zh in range(2)]
                )

            quench_copies = send_around(
                quench_ref, own_quench_strip, near_quench, near_quench_strips, quench_send, quench_recv
            )

    exchange = []
    for d in (4, 5, 3, 6, 2, 7, 1, 0):
        peer = lax.rem(src + d, N_SRC)
        gather(count - 1, waves[(count - 1) % 2], peer)
        if d > 0:
            copy = pltpu.make_async_remote_copy(
                src_ref=planes_ref.at[peer],
                dst_ref=arrived.at[d - 1],
                send_sem=send_sems.at[d - 1],
                recv_sem=recv_sems.at[d - 1],
                device_id=peers[d - 1],
                device_id_type=MESH,
            )
            copy.start()
            exchange.append(copy)

    total = planes_ref[src].astype(jnp.float32)
    for d in range(1, N_SRC):
        exchange[(6, 4, 2, 0, 1, 3, 5)[d - 1]].wait_recv()
        total = total + arrived[d - 1].astype(jnp.float32)
    own_planes[...] = total
    own_strip[...] = packed([own_planes[n * 8 : n * 8 + 8, :] for n in range(PLANES)])
    plane_copies = send_around(
        own_planes, own_strip, near_planes, near_strips, near_send, near_recv
    )

    for copy in quench_copies:
        copy.wait_recv()
    for g in range(3):
        source = quench_ref if g == 1 else near_quench.at[0 if g == 0 else 1]
        for r in range(8):
            field[1, g * 8 + r, :, 0:COLS] = source[r]
        for k in range(2):
            merged = jnp.where(
                first_half, near_quench_strips[2 * g, k], near_quench_strips[2 * g + 1, k]
            )
            for n in range(8):
                row, zh = 4 * k + n // 2, n % 2
                field[1, g * 8 + row, zh * 8 : zh * 8 + 8, COLS : 2 * COLS] = unpacked(
                    merged, n
                )

    z_at = lax.broadcasted_iota(jnp.int32, (DEPTH, COLS), 0).astype(jnp.float32)
    tau = (z_at - 7.5) * (1.0 / 7.5)
    fading = jnp.exp(-ABSORB * z_at)

    def start_acid(g, get, side):
        for r in range(8):
            value = jnp.broadcast_to(get(PLANES - 1)[r : r + 1], (DEPTH, COLS))
            for n in range(PLANES - 2, -1, -1):
                value = value * tau + get(n)[r : r + 1]
            acid = 1.0 - jnp.exp(-value * fading)
            field[0, g * 8 + r, :, side * COLS : (side + 1) * COLS] = acid

    start_acid(1, lambda n: own_planes[n * 8 : n * 8 + 8, :], 0)
    for copy in plane_copies:
        copy.wait_recv()
    for g in range(3):
        if g != 1:
            start_acid(g, lambda n: near_planes[0 if g == 0 else 1, n * 8 : n * 8 + 8, :], 0)
        merged = jnp.where(first_half, near_strips[2 * g], near_strips[2 * g + 1])
        tiles = [unpacked(merged, n) for n in range(PLANES)]
        start_acid(g, lambda n: tiles[n], 1)

    for copy in exchange + quench_copies + plane_copies:
        copy.wait_send()


def halo_field(spectra, shift, offset, weights, codes, levels, quench):
    left, right = wave_tables()
    cell_waves, shape_x, shape_y = cell_tables()
    turn = turn_tables()
    bf16, f32, dma = jnp.bfloat16, jnp.float32, pltpu.SemaphoreType.DMA
    vmem, smem = pltpu.VMEM, pltpu.SMEM
    count = spectra.shape[0]
    return pl.pallas_call(
        image_kernel,
        out_shape=jax.ShapeDtypeStruct((2, 3 * ROWS, DEPTH, 2 * COLS), f32),
        in_specs=[pl.BlockSpec(memory_space=pltpu.HBM)] * 13,
        out_specs=pl.BlockSpec(memory_space=pltpu.VMEM),
        scratch_shapes=[
            smem((2, count), jnp.int32),
            smem((2, count), jnp.int32),
            smem(weights.shape, f32),
            smem(levels.shape, f32),
            vmem(codes.shape, jnp.int32),
            vmem(cell_waves.shape, f32),
            vmem(shape_x.shape, f32),
            vmem(shape_y.shape, f32),
            vmem(turn.shape, f32),
            vmem(left.shape[1:], bf16),
            vmem(right.shape[1:], bf16),
            vmem((2 * N_SRC * ROWS, 2 * WIN), bf16),
            vmem((2 * WIN, 2 * COLS), bf16),
            vmem(spectra.shape, bf16),
            vmem(quench.shape, f32),
            vmem((2, 2 * CELLS, CELLS), f32),
            vmem((3 * TERMS, 2 * WIN, WIN), bf16),
            vmem((3 * TERMS, 2 * WIN, WIN), bf16),
            vmem((3 * TERMS * 64, 2 * WIN), bf16),
            vmem((3 * TERMS * 64, 2 * COLS), f32),
            vmem((3 * TERMS * 64, 2 * COLS), f32),
            vmem((N_SRC, PLANES * ROWS, COLS), f32),
            vmem((N_SRC, PLANES * ROWS, COLS), bf16),
            vmem((N_SRC - 1, PLANES * ROWS, COLS), bf16),
            vmem((PLANES * ROWS, COLS), f32),
            vmem((8, COLS), f32),
            vmem((2, 8, COLS), f32),
            vmem((2, PLANES * ROWS, COLS), f32),
            vmem((6, 8, COLS), f32),
            vmem((2, ROWS, DEPTH, COLS), f32),
            vmem((6, 2, 8, COLS), f32),
            dma((12,)),
            dma((count,)),
            dma((7,)),
            dma((7,)),
            dma((8,)),
            dma((8,)),
            dma((8,)),
            dma((8,)),
        ],
        compiler_params=pltpu.CompilerParams(
            collective_id=0, has_side_effects=True, vmem_limit_bytes=40 << 20
        ),
        name="image",
    )(*(pltpu.with_memory_space_constraint(value, pltpu.HBM) for value in (
        shift.T,
        offset.T,
        weights,
        levels,
        codes,
        jnp.asarray(cell_waves),
        jnp.asarray(shape_x),
        jnp.asarray(shape_y),
        jnp.asarray(turn),
        jnp.asarray(left, bf16),
        jnp.asarray(right, bf16),
        spectra,
        quench,
    )))


def bake_kernel(start, acid_hbm, quench_hbm, inhibit_hbm, field, acid_out, quench_out, inhibit_out, sems):
    z_index = lax.broadcasted_iota(jnp.int32, (DEPTH, 2 * COLS), 0)

    def around_sum(held, which, row):
        here = held[which, row]
        beside = (
            held[which, row - 1]
            + held[which, row + 1]
            + pltpu.roll(here, 1, 1)
            + pltpu.roll(here, 2 * COLS - 1, 1)
        )
        above = jnp.where(z_index == 0, here, pltpu.roll(here, 1, 0))
        below = jnp.where(z_index == DEPTH - 1, here, pltpu.roll(here, DEPTH - 1, 0))
        return here, beside, above + below

    spent = [jnp.zeros((DEPTH, COLS), jnp.float32) for _ in range(ROWS)]
    for step in range(STEPS):
        old = start if step == 0 else field.at[step % 2]
        new = field.at[1 - step % 2]
        last = step == STEPS - 1
        for row in range(step + 1, 23 - step):
            a, a_beside, a_depth = around_sum(old, 0, row)
            q, q_beside, q_depth = around_sum(old, 1, row)
            reaction = 0.08 * a * q
            a_new = 0.1 * a + 0.2 * a_beside + 0.05 * a_depth - reaction
            q_new = 0.73 * q + 0.06 * q_beside + 0.015 * q_depth - reaction
            own = row - 8
            if 0 <= own < ROWS:
                spent[own] = spent[own] + a[:, :COLS]
            if last:
                acid_out[own] = a_new[:, :COLS]
                quench_out[own] = q_new[:, :COLS]
                inhibit_out[own] = jnp.exp(-0.25 * spent[own])
            else:
                new[0, row] = a_new
                new[1, row] = q_new

    copies = [
        pltpu.make_async_copy(source, target, sems.at[i])
        for i, (source, target) in enumerate(
            ((acid_out, acid_hbm), (quench_out, quench_hbm), (inhibit_out, inhibit_hbm))
        )
    ]
    for copy in copies:
        copy.start()
    for copy in copies:
        copy.wait()


def baked(start):
    tile = (ROWS, DEPTH, COLS)
    out = jax.ShapeDtypeStruct(tile, jnp.float32)
    return pl.pallas_call(
        bake_kernel,
        out_shape=(out, out, out),
        in_specs=[pl.BlockSpec(memory_space=pltpu.VMEM)],
        out_specs=(pl.BlockSpec(memory_space=pltpu.HBM),) * 3,
        scratch_shapes=[
            pltpu.VMEM((2, 2, 24, DEPTH, 2 * COLS), jnp.float32),
            pltpu.VMEM(tile, jnp.float32),
            pltpu.VMEM(tile, jnp.float32),
            pltpu.VMEM(tile, jnp.float32),
            pltpu.SemaphoreType.DMA((3,)),
        ],
        compiler_params=pltpu.CompilerParams(vmem_limit_bytes=16 << 20),
        name="bake",
    )(start)


def per_device(
    spectra, pupil_shift, window_offset, source_weight, mask_codes, levels, quench_start
):
    return baked(
        halo_field(
            spectra,
            pupil_shift,
            window_offset,
            source_weight,
            mask_codes,
            levels,
            quench_start,
        )
    )


def solution(mesh):
    in_specs = (
        P("src", None, None, None, None),
        P("src", None),
        P("src", None),
        P(),
        P(),
        P(),
        P(("src", "tx"), None, "ty"),
    )
    out_specs = (
        P(("src", "tx"), None, "ty"),
        P(("src", "tx"), None, "ty"),
        P(("src", "tx"), None, "ty"),
    )
    return jax.shard_map(
        per_device, mesh=mesh, in_specs=in_specs, out_specs=out_specs, check_vma=False
    )
```

```python
import functools
import math

import jax
import jax.numpy as jnp
import numpy as np
from jax import lax
from jax.experimental import pallas as pl
from jax.experimental.pallas import tpu as pltpu
from jax.sharding import PartitionSpec as P

RADIUS = 124
CELL = 4
STEPS = 8
NX = 512
NY = 512
WIN = 256
DEPTH = 16
N_SRC, N_TX, N_TY = 8, 8, 4
ROWS, COLS = 8, 128
CELLS = 128

TWO_PI = 2.0 * math.pi
NUM_AP = 0.33
DZ_WAVE = 0.148
ABSORB = 0.05
NEUTRAL = 0.08

HALF = math.pi * DZ_WAVE * (1.0 - math.sqrt(1.0 - NUM_AP * NUM_AP))
REACH = HALF * 7.5
TERMS = 5
EARLY = 0
REACH_OFF = 3
PLANES = 6
MESH = pl.DeviceIdType.MESH


def fit(function, powers, reach):
    nodes = np.cos((2 * np.arange(400) + 1) * np.pi / 800)
    basis = np.stack([nodes**k for k in powers], 1)
    sides = np.linalg.lstsq(basis, function(reach * nodes), rcond=None)[0]
    return [float(v) for v in sides]


EVEN = fit(np.cos, (0, 2, 4), REACH)
ODD = fit(np.sin, (1, 3), REACH)
SCALE = [EVEN[0], ODD[0], -EVEN[1], -ODD[1], EVEN[2]]


def wave_tables():
    u = np.arange(WIN)
    left = np.zeros((N_TX, 2, N_SRC * ROWS, WIN))
    for tx in range(N_TX):
        local = np.arange(N_SRC * ROWS)
        x = (local // ROWS * N_TX + tx) * ROWS + local % ROWS
        angle = TWO_PI / NX * ((x[:, None] * (u[None, :] - WIN // 2)) % NX)
        c, s = np.cos(angle), np.sin(angle)
        left[tx] = np.stack([c, s])
    right = np.zeros((N_TY, 2, WIN, COLS))
    for ty in range(N_TY):
        y = ty * COLS + np.arange(COLS)
        angle = TWO_PI / NY * ((y[None, :] * (u[:, None] - WIN // 2)) % NY)
        c, s = np.cos(angle), np.sin(angle)
        right[ty] = np.stack([c, s])
    return left, right


def turn_tables():
    fx = np.arange(WIN + 8) - WIN // 2 - REACH_OFF
    fy = np.arange(WIN + 128) - WIN // 2 - REACH_OFF
    radial = fx[:, None] ** 2 + fy[None, :] ** 2
    limit = RADIUS * RADIUS
    axial = np.sqrt(1.0 - (NUM_AP / RADIUS) ** 2 * np.minimum(radial, limit))
    w = TWO_PI * DZ_WAVE * (axial - 1.0) / HALF + 1.0
    inside = radial <= limit
    turn = 8.0 * HALF * w
    table = np.stack([w, np.cos(turn) * inside, np.sin(turn) * inside])
    return np.stack(np.split(table, 3, axis=2), 1).astype(np.float32)


def cell_tables():
    a = np.arange(CELLS)
    angle = TWO_PI / CELLS * ((a[:, None] * a[None, :]) % CELLS)
    c, s = np.cos(angle), np.sin(angle)
    waves = np.stack([c, s]).astype(np.float32)
    high = waves.astype(jnp.bfloat16).astype(np.float32)
    cell_waves = np.stack([high, waves - high])
    orders = np.arange(NX) - NX // 2
    phase = TWO_PI / NX * ((orders[:, None] * np.arange(CELL)[None, :]) % NX)
    shape_re = np.cos(phase).sum(1) / NX
    shape_im = -np.sin(phase).sum(1) / NX
    shape = np.stack([shape_re, shape_im])
    shape_x = np.broadcast_to(shape[:, :, None], (2, NX, 128))
    shape_y = np.broadcast_to(shape[:, None, :], (2, 8, NY))
    return (
        cell_waves,
        shape_x.astype(np.float32),
        shape_y.astype(np.float32),
    )


AROUND = [(dr, dc) for dr in (-1, 0, 1) for dc in (-1, 0, 1) if (dr, dc) != (0, 0)]


def image_kernel(
    shift_hbm,
    offset_hbm,
    weight_hbm,
    levels_hbm,
    codes_hbm,
    cell_waves_hbm,
    shape_x_hbm,
    shape_y_hbm,
    turn_hbm,
    left_hbm,
    right_hbm,
    spectra_hbm,
    quench_hbm,
    field,
    shift_ref,
    offset_ref,
    weight_ref,
    levels_ref,
    codes_ref,
    cell_waves_ref,
    shape_x_ref,
    shape_y_ref,
    turn_ref,
    left_in,
    right_in,
    left_ref,
    right_ref,
    spectra_ref,
    quench_ref,
    cells_ref,
    operand_a,
    operand_b,
    half_ref,
    wave_a,
    wave_b,
    acc_ref,
    planes_ref,
    arrived,
    own_planes,
    own_strip,
    own_quench_strip,
    near_planes,
    near_strips,
    near_quench,
    near_quench_strips,
    load_sems,
    spectra_sems,
    send_sems,
    recv_sems,
    near_send,
    near_recv,
    quench_send,
    quench_recv,
):
    src, tx, ty = lax.axis_index("src"), lax.axis_index("tx"), lax.axis_index("ty")
    place = src * N_TX + tx

    def device_at(dr, dc):
        row = lax.rem(place + dr + N_SRC * N_TX, N_SRC * N_TX)
        column = lax.rem(ty + dc + N_TY, N_TY)
        return (row // N_TX, lax.rem(row, N_TX), column)

    peers = [(lax.rem(src + d, N_SRC), tx, ty) for d in range(1, N_SRC)]
    around = [device_at(dr, dc) for dr, dc in AROUND]

    loads = {}
    pairs = [
        ("codes", codes_hbm, codes_ref),
        ("levels", levels_hbm, levels_ref),
        ("cell", cell_waves_hbm, cell_waves_ref),
        ("shift", shift_hbm, shift_ref),
        ("offset", offset_hbm, offset_ref),
        ("weight", weight_hbm, weight_ref),
        ("shape_x", shape_x_hbm, shape_x_ref),
        ("shape_y", shape_y_hbm, shape_y_ref),
        ("turn", turn_hbm, turn_ref),
        ("left", left_hbm.at[tx], left_in),
        ("right", right_hbm.at[ty], right_in),
        ("quench", quench_hbm, quench_ref),
    ]
    count = spectra_hbm.shape[0]
    spectra_loads = [
        pltpu.make_async_copy(spectra_hbm.at[j], spectra_ref.at[j], spectra_sems.at[j])
        for j in range(count)
    ]
    for i, (name, source, target) in enumerate(pairs):
        loads[name] = pltpu.make_async_copy(source, target, load_sems.at[i])
        loads[name].start()
        if name == "turn":
            spectra_loads[0].start()
    for copy in spectra_loads[1:]:
        copy.start()

    barrier = pltpu.get_barrier_semaphore()
    for device in peers + around:
        pl.semaphore_signal(barrier, inc=1, device_id=device, device_id_type=MESH)

    for name in ("codes", "levels", "cell"):
        loads[name].wait()
    codes = codes_ref[...]
    parts = []
    for part in range(2):
        grid = jnp.full(codes.shape, levels_ref[part, 3], jnp.float32)
        for level in range(3):
            grid = jnp.where(codes == level, levels_ref[part, level], grid)
        parts.append(grid)
    by_column, by_row = [], []
    for part in range(2):
        c, s = cell_waves_ref[part, 0], cell_waves_ref[part, 1]
        by_column.append(
            jnp.concatenate(
                [jnp.concatenate([c, -s], axis=1), jnp.concatenate([s, c], axis=1)], axis=0
            )
        )
        by_row.append(
            jnp.concatenate(
                [jnp.concatenate([c, s], axis=1), jnp.concatenate([-s, c], axis=1)], axis=0
            )
        )
    by_column = jnp.concatenate([by_column[0], by_column[0], by_column[1]], axis=0)
    by_row = jnp.concatenate([by_row[0], by_row[0], by_row[1]], axis=1)
    grid = jnp.concatenate(parts, axis=1)
    high = grid.astype(jnp.bfloat16)
    low = (grid - high.astype(jnp.float32)).astype(jnp.bfloat16)
    across = jnp.dot(
        jnp.concatenate([high, low, high], axis=1),
        by_column,
        preferred_element_type=jnp.float32,
    )
    both = jnp.concatenate([across[:, :CELLS], across[:, CELLS:]], axis=0)
    high = both.astype(jnp.bfloat16)
    low = (both - high.astype(jnp.float32)).astype(jnp.bfloat16)
    full = jnp.dot(
        by_row,
        jnp.concatenate([high, low, high], axis=0),
        preferred_element_type=jnp.float32,
    )
    for part in range(2):
        piece = full[part * CELLS : (part + 1) * CELLS]
        cells_ref[part, 0:CELLS] = piece
        cells_ref[part, CELLS : 2 * CELLS] = piece
    for name in ("shift", "offset", "weight", "shape_x", "shape_y", "turn", "left", "right"):
        loads[name].wait()

    rows = N_SRC * ROWS
    left_ref[0:rows, 0:WIN] = left_in[0]
    left_ref[0:rows, WIN : 2 * WIN] = -left_in[1]
    left_ref[rows : 2 * rows, 0:WIN] = left_in[1]
    left_ref[rows : 2 * rows, WIN : 2 * WIN] = left_in[0]
    right_ref[0:WIN, 0:COLS] = right_in[0]
    right_ref[0:WIN, COLS : 2 * COLS] = right_in[1]
    right_ref[WIN : 2 * WIN, 0:COLS] = -right_in[1]
    right_ref[WIN : 2 * WIN, COLS : 2 * COLS] = right_in[0]

    total_weight = weight_ref[0]
    for k in range(1, weight_ref.shape[0]):
        total_weight = total_weight + weight_ref[k]
    norm = 1.0 / jnp.full((ROWS, COLS), total_weight, jnp.float32)

    def builder(j, operand):
        spectra_loads[j].wait()
        off_x, off_y = offset_ref[0, j], offset_ref[1, j]
        start_x = off_x - shift_ref[0, j] - WIN // 2 + NX // 2
        start_y = off_y - shift_ref[1, j] - WIN // 2 + NY // 2
        cell_x = lax.rem(start_x, CELLS)
        roll_y = lax.rem(2 * CELLS - lax.rem(start_y, CELLS), CELLS)
        turn_x = off_x + REACH_OFF
        turn_y = lax.rem(COLS - (off_y + REACH_OFF), COLS)
        shape_y = [
            pltpu.roll(shape_y_ref[part], NY - start_y, 1)[:, :WIN] for part in range(2)
        ]
        y_both = [jnp.concatenate([value] * 2, axis=0) for value in shape_y]

        lane = lax.broadcasted_iota(jnp.int32, (16, COLS), 1)
        kept = lane < COLS - (off_y + REACH_OFF)

        def turned(k, at):
            moved = [
                pltpu.roll(turn_ref[k, t, pl.ds(turn_x + at, 16), :], turn_y, 1)
                for t in range(3)
            ]
            return [jnp.where(kept, moved[t], moved[t + 1]) for t in range(2)]

        def build(step):
            at = step * 16 if isinstance(step, int) else pl.multiple_of(step * 16, 16)
            cell_at = lax.rem(cell_x + at, CELLS)
            g_re = pltpu.roll(cells_ref[0, pl.ds(cell_at, 16), :], roll_y, 1)
            g_im = pltpu.roll(cells_ref[1, pl.ds(cell_at, 16), :], roll_y, 1)
            x_re = shape_x_ref[0, pl.ds(start_x + at, 16), :]
            x_im = shape_x_ref[1, pl.ds(start_x + at, 16), :]
            gx_re = g_re * x_re - g_im * x_im
            gx_im = g_re * x_im + g_im * x_re
            w_both, turn_re_both, turn_im_both = (turned(k, at) for k in range(3))
            w = jnp.concatenate(w_both, axis=1).astype(jnp.bfloat16)
            turn_re = jnp.concatenate(turn_re_both, axis=1)
            turn_im = jnp.concatenate(turn_im_both, axis=1)
            gx_re = jnp.concatenate([gx_re, gx_re], axis=1)
            gx_im = jnp.concatenate([gx_im, gx_im], axis=1)
            y_re, y_im = y_both
            thin_re = gx_re * y_re - gx_im * y_im
            thin_im = gx_re * y_im + gx_im * y_re
            h_re = thin_re * turn_re - thin_im * turn_im
            h_im = thin_re * turn_im + thin_im * turn_re
            for c in range(3):
                f_re = spectra_ref[j, c, 0, pl.ds(at, 16), :].astype(jnp.float32)
                f_im = spectra_ref[j, c, 1, pl.ds(at, 16), :].astype(jnp.float32)
                s_re = (f_re * h_re - f_im * h_im).astype(jnp.bfloat16)
                s_im = (f_re * h_im + f_im * h_re).astype(jnp.bfloat16)
                for n in range(TERMS):
                    operand[c * TERMS + n, pl.ds(at, 16), :] = s_re
                    operand[c * TERMS + n, pl.ds(WIN + at, 16), :] = s_im
                    if n < TERMS - 1:
                        s_re = s_re * w
                        s_im = s_im * w

        return build

    def first(operand, block):
        halves = jnp.dot(
            left_ref[...], operand[block], preferred_element_type=jnp.float32
        ).astype(jnp.bfloat16)
        half_ref[block * 64 : (block + 1) * 64, 0:WIN] = halves[0:64]
        half_ref[block * 64 : (block + 1) * 64, WIN : 2 * WIN] = halves[64:128]

    def second(wave, c):
        span = slice(c * TERMS * 64, (c + 1) * TERMS * 64)
        wave[span, :] = jnp.dot(
            half_ref[span, :], right_ref[...], preferred_element_type=jnp.float32
        )

    def gather(j, wave, p):
        at = p * ROWS
        if j == count - 1:
            at = pl.multiple_of(at, ROWS)
        weight = weight_ref[src * count + j] * norm
        real = ((0, 0), (1, 1), (0, 2), (2, 2), (0, 4), (1, 3), (3, 3), (2, 4), (4, 4))
        imag = ((1, 0), (1, 2), (3, 0), (1, 4), (3, 2), (3, 4))
        total = {}
        for c in range(3):
            re, im = [], []
            for n in range(TERMS):
                rows = pl.ds((c * TERMS + n) * 64 + at, ROWS)
                re.append(wave[rows, 0:COLS])
                im.append(wave[rows, COLS : 2 * COLS])
            for a, b in real:
                value = re[a] * re[b] + im[a] * im[b]
                total[a, b] = value if c == 0 else total[a, b] + value
            for a, b in imag:
                value = im[a] * re[b] - re[a] * im[b]
                total[-a - 1, b] = value if c == 0 else total[-a - 1, b] + value

        def part(a, b, factor):
            sign = a if a >= 0 else -a - 1
            return total[a, b] * (weight * (factor * SCALE[sign] * SCALE[b]))

        eighth = part(4, 4, 1.0)
        seventh = part(-4, 4, 2.0)
        sixth = part(3, 3, 1.0) + part(2, 4, -2.0) + 2.0 * eighth
        planes = [
            part(0, 0, 1.0) + sixth * (1.0 / 32.0) - eighth * (1.0 / 128.0),
            part(-2, 0, -2.0) + seventh * (7.0 / 64.0),
            part(1, 1, 1.0) + part(0, 2, -2.0) + eighth * 0.25 - sixth * 0.5625,
            part(-2, 2, 2.0) + part(-4, 0, 2.0) - seventh * 0.875,
            part(2, 2, 1.0) + part(0, 4, 2.0) + part(1, 3, -2.0) + sixth * 1.5 - eighth * 1.25,
            part(-2, 4, -2.0) + part(-4, 2, -2.0) + seventh * 1.75,
        ]
        if j > 0:
            planes = [
                planes[n] + acc_ref[p, n * ROWS : (n + 1) * ROWS, :] for n in range(PLANES)
            ]
        if j < count - 1:
            for n in range(PLANES):
                acc_ref[p, n * ROWS : (n + 1) * ROWS, :] = planes[n]
        else:
            planes_ref[p] = jnp.concatenate(planes[:PLANES], axis=0).astype(jnp.bfloat16)

    lane = lax.broadcasted_iota(jnp.int32, (8, COLS), 1)
    group = lane // 16

    def packed(tiles):
        total = jnp.zeros((8, COLS), jnp.float32)
        for n, tile in enumerate(tiles):
            moved = pltpu.roll(tile, (8 + 16 * n) % COLS, 1)
            total = jnp.where(group == n, moved, total)
        return total

    def unpacked(merged, n):
        tile = pltpu.roll(merged, (COLS - 8 - 16 * n) % COLS, 1)
        return jnp.where((lane < 8) | (lane >= COLS - 8), tile, 0.0)

    first_half = lax.rem(lane, 16) < 8

    def send_around(rows, whole, strip, near_whole, near_strip, sends, recvs):
        copies = []
        for i, (dr, dc) in enumerate(AROUND):
            if (dc == 0) != rows:
                continue
            if dc == 0:
                source, target = whole, near_whole.at[0 if dr == 1 else 1]
            else:
                slot = (1 - dr) * 2 + (0 if dc == 1 else 1)
                source, target = strip, near_strip.at[slot]
            copy = pltpu.make_async_remote_copy(
                src_ref=source,
                dst_ref=target,
                send_sem=sends.at[i],
                recv_sem=recvs.at[i],
                device_id=around[i],
                device_id_type=MESH,
            )
            copy.start()
            copies.append(copy)
        return copies

    operands = (operand_a, operand_b)
    waves = (wave_a, wave_b)
    build = builder(0, operands[0])

    @pl.loop(0, 4)
    def _(quad):
        for b in range(4):
            build(quad * 4 + b)

    for j in range(count):
        build = builder(j + 1, operands[(j + 1) % 2]) if j + 1 < count else None
        for step in range(WIN // 16):
            if step < 3 * TERMS:
                first(operands[j % 2], step)
            if build is not None:
                build(step)
            if j > 0 and step % 2 == 0:
                gather(j - 1, waves[(j - 1) % 2], step // 2)
            if step in (5, 10, 15):
                second(waves[j % 2], step // 5 - 1)
        if j == EARLY:
            pl.semaphore_wait(barrier, len(peers) + len(around))
            loads["quench"].wait()
            for k in range(2):
                own_quench_strip[k] = packed(
                    [quench_ref[r, zh * 8 : zh * 8 + 8, :] for r in range(4 * k, 4 * k + 4) for zh in range(2)]
                )

            quench_copies = []
            for rows in (True, False):
                quench_copies += send_around(
                    rows,
                    quench_ref,
                    own_quench_strip,
                    near_quench,
                    near_quench_strips,
                    quench_send,
                    quench_recv,
                )

    exchange = []
    for d in (4, 5, 3, 6, 2, 7, 1, 0):
        peer = lax.rem(src + d, N_SRC)
        gather(count - 1, waves[(count - 1) % 2], peer)
        if d > 0:
            copy = pltpu.make_async_remote_copy(
                src_ref=planes_ref.at[peer],
                dst_ref=arrived.at[d - 1],
                send_sem=send_sems.at[d - 1],
                recv_sem=recv_sems.at[d - 1],
                device_id=peers[d - 1],
                device_id_type=MESH,
            )
            copy.start()
            exchange.append(copy)

    total = planes_ref[src].astype(jnp.float32)
    for d in range(1, N_SRC):
        exchange[(6, 4, 2, 0, 1, 3, 5)[d - 1]].wait_recv()
        total = total + arrived[d - 1].astype(jnp.float32)
    own_planes[...] = total
    near = (own_planes, own_strip, near_planes, near_strips, near_send, near_recv)
    row_copies = send_around(True, *near)
    own_strip[...] = packed([total[n * 8 : n * 8 + 8, :] for n in range(PLANES)])
    strip_copies = send_around(False, *near)
    plane_copies = row_copies + strip_copies

    for copy in quench_copies:
        copy.wait_recv()
    for g in range(3):
        source = quench_ref if g == 1 else near_quench.at[0 if g == 0 else 1]
        for r in range(8):
            field[1, g * 8 + r, :, 0:COLS] = NEUTRAL * source[r]
        for k in range(2):
            merged = jnp.where(
                first_half, near_quench_strips[2 * g, k], near_quench_strips[2 * g + 1, k]
            )
            for n in range(8):
                row, zh = 4 * k + n // 2, n % 2
                field[1, g * 8 + row, zh * 8 : zh * 8 + 8, COLS : 2 * COLS] = (
                    NEUTRAL * unpacked(merged, n)
                )

    z_at = lax.broadcasted_iota(jnp.int32, (DEPTH, COLS), 0).astype(jnp.float32)
    tau = (z_at - 7.5) * (1.0 / 7.5)
    fading = jnp.exp(-ABSORB * z_at)

    def start_acid(g, get, side):
        for r in range(8):
            value = jnp.broadcast_to(get(PLANES - 1)[r : r + 1], (DEPTH, COLS))
            for n in range(PLANES - 2, -1, -1):
                value = value * tau + get(n)[r : r + 1]
            acid = NEUTRAL - NEUTRAL * jnp.exp(-value * fading)
            field[0, g * 8 + r, :, side * COLS : (side + 1) * COLS] = acid

    start_acid(1, lambda n: own_planes[n * 8 : n * 8 + 8, :], 0)
    for copy in row_copies:
        copy.wait_recv()
    for g in (0, 2):
        start_acid(g, lambda n: near_planes[g // 2, n * 8 : n * 8 + 8, :], 0)
    for copy in strip_copies:
        copy.wait_recv()
    for g in range(3):
        merged = jnp.where(first_half, near_strips[2 * g], near_strips[2 * g + 1])
        tiles = [unpacked(merged, n) for n in range(PLANES)]
        start_acid(g, lambda n: tiles[n], 1)

    for copy in exchange + quench_copies + plane_copies:
        copy.wait_send()


def halo_field(spectra, shift, offset, weights, codes, levels, quench):
    left, right = wave_tables()
    cell_waves, shape_x, shape_y = cell_tables()
    turn = turn_tables()
    bf16, f32, dma = jnp.bfloat16, jnp.float32, pltpu.SemaphoreType.DMA
    vmem, smem = pltpu.VMEM, pltpu.SMEM
    count = spectra.shape[0]
    return pl.pallas_call(
        image_kernel,
        out_shape=jax.ShapeDtypeStruct((2, 3 * ROWS, DEPTH, 2 * COLS), f32),
        in_specs=[pl.BlockSpec(memory_space=pltpu.HBM)] * 13,
        out_specs=pl.BlockSpec(memory_space=pltpu.VMEM),
        scratch_shapes=[
            smem((2, count), jnp.int32),
            smem((2, count), jnp.int32),
            smem(weights.shape, f32),
            smem(levels.shape, f32),
            vmem(codes.shape, jnp.int32),
            vmem(cell_waves.shape, bf16),
            vmem(shape_x.shape, f32),
            vmem(shape_y.shape, f32),
            vmem(turn.shape, f32),
            vmem(left.shape[1:], bf16),
            vmem(right.shape[1:], bf16),
            vmem((2 * N_SRC * ROWS, 2 * WIN), bf16),
            vmem((2 * WIN, 2 * COLS), bf16),
            vmem(spectra.shape, bf16),
            vmem(quench.shape, f32),
            vmem((2, 2 * CELLS, CELLS), f32),
            vmem((3 * TERMS, 2 * WIN, WIN), bf16),
            vmem((3 * TERMS, 2 * WIN, WIN), bf16),
            vmem((3 * TERMS * 64, 2 * WIN), bf16),
            vmem((3 * TERMS * 64, 2 * COLS), f32),
            vmem((3 * TERMS * 64, 2 * COLS), f32),
            vmem((N_SRC, PLANES * ROWS, COLS), f32),
            vmem((N_SRC, PLANES * ROWS, COLS), bf16),
            vmem((N_SRC - 1, PLANES * ROWS, COLS), bf16),
            vmem((PLANES * ROWS, COLS), f32),
            vmem((8, COLS), f32),
            vmem((2, 8, COLS), f32),
            vmem((2, PLANES * ROWS, COLS), f32),
            vmem((6, 8, COLS), f32),
            vmem((2, ROWS, DEPTH, COLS), f32),
            vmem((6, 2, 8, COLS), f32),
            dma((12,)),
            dma((count,)),
            dma((7,)),
            dma((7,)),
            dma((8,)),
            dma((8,)),
            dma((8,)),
            dma((8,)),
        ],
        compiler_params=pltpu.CompilerParams(
            collective_id=0, has_side_effects=True, vmem_limit_bytes=40 << 20
        ),
        name="image",
    )(*(pltpu.with_memory_space_constraint(value, pltpu.HBM) for value in (
        shift.T,
        offset.T,
        weights,
        levels,
        codes,
        jnp.asarray(cell_waves, bf16),
        jnp.asarray(shape_x),
        jnp.asarray(shape_y),
        jnp.asarray(turn),
        jnp.asarray(left, bf16),
        jnp.asarray(right, bf16),
        spectra,
        quench,
    )))


def bake_kernel(start, acid_hbm, quench_hbm, inhibit_hbm, field, acid_out, quench_out, inhibit_out, sems):
    shape = (DEPTH // 2, COLS)
    lane = lax.broadcasted_iota(jnp.int32, shape, 1)
    depth = lax.broadcasted_iota(jnp.int32, shape, 0)
    first_lane, last_lane = lane == 0, lane == COLS - 1
    top, bottom = depth == 0, depth == DEPTH // 2 - 1

    def halves(held, which, row):
        return [
            [held[which, row, z : z + 8, t : t + COLS] for t in (0, COLS)] for z in (0, 8)
        ]

    def sums(held, which, row, sides):
        before, here, after = (halves(held, which, row + k) for k in (-1, 0, 1))
        out = []
        for t in range(sides):
            low, high = here[0][t], here[1][t]
            low_up, high_up = pltpu.roll(low, 1, 0), pltpu.roll(high, 1, 0)
            low_down, high_down = pltpu.roll(low, 7, 0), pltpu.roll(high, 7, 0)
            along = (
                jnp.where(top, low, low_up) + jnp.where(bottom, high_down, low_down),
                jnp.where(top, low_up, high_up) + jnp.where(bottom, high, high_down),
            )
            for z in range(2):
                mine, other = here[z][t], here[z][1 - t]
                left = jnp.where(first_lane, pltpu.roll(other, 1, 1), pltpu.roll(mine, 1, 1))
                right = jnp.where(
                    last_lane, pltpu.roll(other, COLS - 1, 1), pltpu.roll(mine, COLS - 1, 1)
                )
                beside = (before[z][t] + after[z][t]) + (left + right)
                out.append((z, t, mine, beside + 0.25 * along[z]))
        return out

    copies = []

    def send(part):
        rows = pl.ds(part * 4, 4)
        for i, (source, target) in enumerate(
            ((acid_out, acid_hbm), (quench_out, quench_hbm), (inhibit_out, inhibit_hbm))
        ):
            copy = pltpu.make_async_copy(
                source.at[rows], target.at[rows], sems.at[part * 3 + i]
            )
            copy.start()
            copies.append(copy)

    spent = {}
    for step in range(STEPS):
        old = start if step == 0 else field.at[step % 2]
        new = field.at[1 - step % 2]
        last = step == STEPS - 1
        for row in range(step + 1, 23 - step):
            sides = 1 if last or row in (step + 1, 22 - step) else 2
            own = row - 8
            for (z, t, a, a_sum), (_, _, q, q_sum) in zip(
                sums(old, 0, row, sides), sums(old, 1, row, sides)
            ):
                a_new = a * (0.1 - q) + 0.2 * a_sum
                q_new = q * (0.73 - a) + 0.06 * q_sum
                span = slice(z * 8, z * 8 + 8)
                if 0 <= own < ROWS and t == 0:
                    spent[own, z] = spent[own, z] + a if step else a
                if last:
                    acid_out[own, span] = a_new * (1.0 / NEUTRAL)
                    quench_out[own, span] = q_new * (1.0 / NEUTRAL)
                    inhibit_out[own, span] = jnp.exp((-0.25 / NEUTRAL) * spent[own, z])
                else:
                    lanes = slice(t * COLS, (t + 1) * COLS)
                    new[0, row, span, lanes] = a_new
                    new[1, row, span, lanes] = q_new
            if last and own % 4 == 3:
                send(own // 4)

    for copy in copies:
        copy.wait()


def baked(start):
    tile = (ROWS, DEPTH, COLS)
    out = jax.ShapeDtypeStruct(tile, jnp.float32)
    return pl.pallas_call(
        bake_kernel,
        out_shape=(out, out, out),
        in_specs=[pl.BlockSpec(memory_space=pltpu.VMEM)],
        out_specs=(pl.BlockSpec(memory_space=pltpu.HBM),) * 3,
        scratch_shapes=[
            pltpu.VMEM((2, 2, 24, DEPTH, 2 * COLS), jnp.float32),
            pltpu.VMEM(tile, jnp.float32),
            pltpu.VMEM(tile, jnp.float32),
            pltpu.VMEM(tile, jnp.float32),
            pltpu.SemaphoreType.DMA((6,)),
        ],
        compiler_params=pltpu.CompilerParams(vmem_limit_bytes=16 << 20),
        name="bake",
    )(start)


def per_device(
    spectra, pupil_shift, window_offset, source_weight, mask_codes, levels, quench_start
):
    return baked(
        halo_field(
            spectra,
            pupil_shift,
            window_offset,
            source_weight,
            mask_codes,
            levels,
            quench_start,
        )
    )


def solution(mesh):
    in_specs = (
        P("src", None, None, None, None),
        P("src", None),
        P("src", None),
        P(),
        P(),
        P(),
        P(("src", "tx"), None, "ty"),
    )
    out_specs = (
        P(("src", "tx"), None, "ty"),
        P(("src", "tx"), None, "ty"),
        P(("src", "tx"), None, "ty"),
    )
    return jax.shard_map(
        per_device, mesh=mesh, in_specs=in_specs, out_specs=out_specs, check_vma=False
    )
```

```python
import functools
import math

import jax
import jax.numpy as jnp
import numpy as np
from jax import lax
from jax.experimental import pallas as pl
from jax.experimental.pallas import tpu as pltpu
from jax.sharding import PartitionSpec as P

RADIUS = 124
CELL = 4
STEPS = 8
NX = 512
NY = 512
WIN = 256
DEPTH = 16
N_SRC, N_TX, N_TY = 8, 8, 4
ROWS, COLS = 8, 128
CELLS = 128

TWO_PI = 2.0 * math.pi
NUM_AP = 0.33
DZ_WAVE = 0.148
ABSORB = 0.05
NEUTRAL = 0.08

HALF = math.pi * DZ_WAVE * (1.0 - math.sqrt(1.0 - NUM_AP * NUM_AP))
REACH = HALF * 7.5
TERMS = 5
EARLY = 0
REACH_OFF = 3
PLANES = 6
MESH = pl.DeviceIdType.MESH


def fit(function, powers, reach):
    nodes = np.cos((2 * np.arange(400) + 1) * np.pi / 800)
    basis = np.stack([nodes**k for k in powers], 1)
    sides = np.linalg.lstsq(basis, function(reach * nodes), rcond=None)[0]
    return [float(v) for v in sides]


EVEN = fit(np.cos, (0, 2, 4), REACH)
ODD = fit(np.sin, (1, 3), REACH)
SCALE = [EVEN[0], ODD[0], -EVEN[1], -ODD[1], EVEN[2]]


def wave_tables():
    u = np.arange(WIN)
    left = np.zeros((N_TX, 2, N_SRC * ROWS, WIN))
    for tx in range(N_TX):
        local = np.arange(N_SRC * ROWS)
        x = (local // ROWS * N_TX + tx) * ROWS + local % ROWS
        angle = TWO_PI / NX * ((x[:, None] * (u[None, :] - WIN // 2)) % NX)
        c, s = np.cos(angle), np.sin(angle)
        left[tx] = np.stack([c, s])
    right = np.zeros((N_TY, 2, WIN, COLS))
    for ty in range(N_TY):
        y = ty * COLS + np.arange(COLS)
        angle = TWO_PI / NY * ((y[None, :] * (u[:, None] - WIN // 2)) % NY)
        c, s = np.cos(angle), np.sin(angle)
        right[ty] = np.stack([c, s])
    return left, right


def turn_tables():
    fx = np.arange(WIN + 8) - WIN // 2 - REACH_OFF
    fy = np.arange(WIN + 128) - WIN // 2 - REACH_OFF
    radial = fx[:, None] ** 2 + fy[None, :] ** 2
    limit = RADIUS * RADIUS
    axial = np.sqrt(1.0 - (NUM_AP / RADIUS) ** 2 * np.minimum(radial, limit))
    w = TWO_PI * DZ_WAVE * (axial - 1.0) / HALF + 1.0
    inside = radial <= limit
    turn = 8.0 * HALF * w
    table = np.stack([w, np.cos(turn) * inside, np.sin(turn) * inside])
    return np.stack(np.split(table, 3, axis=2), 1).astype(np.float32)


def cell_tables():
    a = np.arange(CELLS)
    angle = TWO_PI / CELLS * ((a[:, None] * a[None, :]) % CELLS)
    c, s = np.cos(angle), np.sin(angle)
    waves = np.stack([c, s]).astype(np.float32)
    high = waves.astype(jnp.bfloat16).astype(np.float32)
    cell_waves = np.stack([high, waves - high])
    orders = np.arange(NX) - NX // 2
    phase = TWO_PI / NX * ((orders[:, None] * np.arange(CELL)[None, :]) % NX)
    shape_re = np.cos(phase).sum(1) / NX
    shape_im = -np.sin(phase).sum(1) / NX
    shape = np.stack([shape_re, shape_im])
    shape_x = np.broadcast_to(shape[:, :, None], (2, NX, 128))
    shape_y = np.broadcast_to(shape[:, None, :], (2, 8, NY))
    return (
        cell_waves,
        shape_x.astype(np.float32),
        shape_y.astype(np.float32),
    )


AROUND = [(-1, -1), (-1, 1), (1, -1), (1, 1), (0, -1), (0, 1), (-1, 0), (1, 0)]


def image_kernel(
    shift_hbm,
    offset_hbm,
    weight_hbm,
    levels_hbm,
    codes_hbm,
    cell_waves_hbm,
    shape_x_hbm,
    shape_y_hbm,
    turn_hbm,
    left_hbm,
    right_hbm,
    spectra_hbm,
    quench_hbm,
    field,
    shift_ref,
    offset_ref,
    weight_ref,
    levels_ref,
    codes_ref,
    cell_waves_ref,
    shape_x_ref,
    shape_y_ref,
    turn_ref,
    left_in,
    right_in,
    left_ref,
    right_ref,
    spectra_ref,
    quench_ref,
    cells_ref,
    operand_a,
    operand_b,
    half_ref,
    wave_a,
    wave_b,
    acc_ref,
    planes_ref,
    arrived,
    own_planes,
    own_strip,
    own_quench_strip,
    near_planes,
    near_strips,
    near_quench,
    near_quench_strips,
    load_sems,
    spectra_sems,
    send_sems,
    recv_sems,
    near_send,
    near_recv,
    quench_send,
    quench_recv,
):
    src, tx, ty = lax.axis_index("src"), lax.axis_index("tx"), lax.axis_index("ty")
    place = src * N_TX + tx

    def device_at(dr, dc):
        row = lax.rem(place + dr + N_SRC * N_TX, N_SRC * N_TX)
        column = lax.rem(ty + dc + N_TY, N_TY)
        return (row // N_TX, lax.rem(row, N_TX), column)

    peers = [(lax.rem(src + d, N_SRC), tx, ty) for d in range(1, N_SRC)]
    around = [device_at(dr, dc) for dr, dc in AROUND]

    loads = {}
    pairs = [
        ("codes", codes_hbm, codes_ref),
        ("levels", levels_hbm, levels_ref),
        ("cell", cell_waves_hbm, cell_waves_ref),
        ("shift", shift_hbm, shift_ref),
        ("offset", offset_hbm, offset_ref),
        ("weight", weight_hbm, weight_ref),
        ("shape_x", shape_x_hbm, shape_x_ref),
        ("shape_y", shape_y_hbm, shape_y_ref),
        ("turn", turn_hbm, turn_ref),
        ("left", left_hbm.at[tx], left_in),
        ("right", right_hbm.at[ty], right_in),
        ("quench", quench_hbm, quench_ref),
    ]
    count = spectra_hbm.shape[0]
    spectra_loads = [
        pltpu.make_async_copy(spectra_hbm.at[j], spectra_ref.at[j], spectra_sems.at[j])
        for j in range(count)
    ]
    for i, (name, source, target) in enumerate(pairs):
        loads[name] = pltpu.make_async_copy(source, target, load_sems.at[i])
        loads[name].start()
        if name == "turn":
            spectra_loads[0].start()
    for copy in spectra_loads[1:]:
        copy.start()

    barrier = pltpu.get_barrier_semaphore()
    for device in peers + around:
        pl.semaphore_signal(barrier, inc=1, device_id=device, device_id_type=MESH)

    for name in ("codes", "levels", "cell"):
        loads[name].wait()
    codes = codes_ref[...]
    parts = []
    for part in range(2):
        grid = jnp.full(codes.shape, levels_ref[part, 3], jnp.float32)
        for level in range(3):
            grid = jnp.where(codes == level, levels_ref[part, level], grid)
        parts.append(grid)
    by_column, by_row = [], []
    for part in range(2):
        c, s = cell_waves_ref[part, 0], cell_waves_ref[part, 1]
        by_column.append(
            jnp.concatenate(
                [jnp.concatenate([c, -s], axis=1), jnp.concatenate([s, c], axis=1)], axis=0
            )
        )
        by_row.append(
            jnp.concatenate(
                [jnp.concatenate([c, s], axis=1), jnp.concatenate([-s, c], axis=1)], axis=0
            )
        )
    by_column = jnp.concatenate([by_column[0], by_column[0], by_column[1]], axis=0)
    by_row = jnp.concatenate([by_row[0], by_row[0], by_row[1]], axis=1)
    grid = jnp.concatenate(parts, axis=1)
    high = grid.astype(jnp.bfloat16)
    low = (grid - high.astype(jnp.float32)).astype(jnp.bfloat16)
    across = jnp.dot(
        jnp.concatenate([high, low, high], axis=1),
        by_column,
        preferred_element_type=jnp.float32,
    )
    both = jnp.concatenate([across[:, :CELLS], across[:, CELLS:]], axis=0)
    high = both.astype(jnp.bfloat16)
    low = (both - high.astype(jnp.float32)).astype(jnp.bfloat16)
    full = jnp.dot(
        by_row,
        jnp.concatenate([high, low, high], axis=0),
        preferred_element_type=jnp.float32,
    )
    for part in range(2):
        piece = full[part * CELLS : (part + 1) * CELLS]
        cells_ref[part, 0:CELLS] = piece
        cells_ref[part, CELLS : 2 * CELLS] = piece
    for name in ("shift", "offset", "weight", "shape_x", "shape_y", "turn", "left", "right"):
        loads[name].wait()

    rows = N_SRC * ROWS
    left_ref[0:rows, 0:WIN] = left_in[0]
    left_ref[0:rows, WIN : 2 * WIN] = -left_in[1]
    left_ref[rows : 2 * rows, 0:WIN] = left_in[1]
    left_ref[rows : 2 * rows, WIN : 2 * WIN] = left_in[0]
    right_ref[0:WIN, 0:COLS] = right_in[0]
    right_ref[0:WIN, COLS : 2 * COLS] = right_in[1]
    right_ref[WIN : 2 * WIN, 0:COLS] = -right_in[1]
    right_ref[WIN : 2 * WIN, COLS : 2 * COLS] = right_in[0]

    total_weight = weight_ref[0]
    for k in range(1, weight_ref.shape[0]):
        total_weight = total_weight + weight_ref[k]
    norm = 1.0 / jnp.full((ROWS, COLS), total_weight, jnp.float32)

    def builder(j, operand):
        spectra_loads[j].wait()
        off_x, off_y = offset_ref[0, j], offset_ref[1, j]
        start_x = off_x - shift_ref[0, j] - WIN // 2 + NX // 2
        start_y = off_y - shift_ref[1, j] - WIN // 2 + NY // 2
        cell_x = lax.rem(start_x, CELLS)
        roll_y = lax.rem(2 * CELLS - lax.rem(start_y, CELLS), CELLS)
        turn_x = off_x + REACH_OFF
        turn_y = lax.rem(COLS - (off_y + REACH_OFF), COLS)
        shape_y = [
            pltpu.roll(shape_y_ref[part], NY - start_y, 1)[:, :WIN] for part in range(2)
        ]
        y_both = [jnp.concatenate([value] * 2, axis=0) for value in shape_y]

        lane = lax.broadcasted_iota(jnp.int32, (16, COLS), 1)
        kept = lane < COLS - (off_y + REACH_OFF)

        def turned(k, at):
            moved = [
                pltpu.roll(turn_ref[k, t, pl.ds(turn_x + at, 16), :], turn_y, 1)
                for t in range(3)
            ]
            return [jnp.where(kept, moved[t], moved[t + 1]) for t in range(2)]

        def build(step):
            at = step * 16 if isinstance(step, int) else pl.multiple_of(step * 16, 16)
            cell_at = lax.rem(cell_x + at, CELLS)
            g_re = pltpu.roll(cells_ref[0, pl.ds(cell_at, 16), :], roll_y, 1)
            g_im = pltpu.roll(cells_ref[1, pl.ds(cell_at, 16), :], roll_y, 1)
            x_re = shape_x_ref[0, pl.ds(start_x + at, 16), :]
            x_im = shape_x_ref[1, pl.ds(start_x + at, 16), :]
            gx_re = g_re * x_re - g_im * x_im
            gx_im = g_re * x_im + g_im * x_re
            w_both, turn_re_both, turn_im_both = (turned(k, at) for k in range(3))
            w = jnp.concatenate(w_both, axis=1).astype(jnp.bfloat16)
            turn_re = jnp.concatenate(turn_re_both, axis=1)
            turn_im = jnp.concatenate(turn_im_both, axis=1)
            gx_re = jnp.concatenate([gx_re, gx_re], axis=1)
            gx_im = jnp.concatenate([gx_im, gx_im], axis=1)
            y_re, y_im = y_both
            thin_re = gx_re * y_re - gx_im * y_im
            thin_im = gx_re * y_im + gx_im * y_re
            h_re = thin_re * turn_re - thin_im * turn_im
            h_im = thin_re * turn_im + thin_im * turn_re
            for c in range(3):
                f_re = spectra_ref[j, c, 0, pl.ds(at, 16), :].astype(jnp.float32)
                f_im = spectra_ref[j, c, 1, pl.ds(at, 16), :].astype(jnp.float32)
                s_re = (f_re * h_re - f_im * h_im).astype(jnp.bfloat16)
                s_im = (f_re * h_im + f_im * h_re).astype(jnp.bfloat16)
                for n in range(TERMS):
                    operand[c * TERMS + n, pl.ds(at, 16), :] = s_re
                    operand[c * TERMS + n, pl.ds(WIN + at, 16), :] = s_im
                    if n < TERMS - 1:
                        s_re = s_re * w
                        s_im = s_im * w

        return build

    def first(operand, block):
        halves = jnp.dot(
            left_ref[...], operand[block], preferred_element_type=jnp.float32
        ).astype(jnp.bfloat16)
        half_ref[block * 64 : (block + 1) * 64, 0:WIN] = halves[0:64]
        half_ref[block * 64 : (block + 1) * 64, WIN : 2 * WIN] = halves[64:128]

    def second(wave, c):
        span = slice(c * TERMS * 64, (c + 1) * TERMS * 64)
        wave[span, :] = jnp.dot(
            half_ref[span, :], right_ref[...], preferred_element_type=jnp.float32
        )

    def gather(j, wave, p):
        at = p * ROWS
        if j == count - 1:
            at = pl.multiple_of(at, ROWS)
        weight = weight_ref[src * count + j] * norm
        real = ((0, 0), (1, 1), (0, 2), (2, 2), (0, 4), (1, 3), (3, 3), (2, 4), (4, 4))
        imag = ((1, 0), (1, 2), (3, 0), (1, 4), (3, 2), (3, 4))
        total = {}
        for c in range(3):
            re, im = [], []
            for n in range(TERMS):
                rows = pl.ds((c * TERMS + n) * 64 + at, ROWS)
                re.append(wave[rows, 0:COLS])
                im.append(wave[rows, COLS : 2 * COLS])
            for a, b in real:
                value = re[a] * re[b] + im[a] * im[b]
                total[a, b] = value if c == 0 else total[a, b] + value
            for a, b in imag:
                value = im[a] * re[b] - re[a] * im[b]
                total[-a - 1, b] = value if c == 0 else total[-a - 1, b] + value

        def part(a, b, factor):
            sign = a if a >= 0 else -a - 1
            return total[a, b] * (weight * (factor * SCALE[sign] * SCALE[b]))

        eighth = part(4, 4, 1.0)
        seventh = part(-4, 4, 2.0)
        sixth = part(3, 3, 1.0) + part(2, 4, -2.0) + 2.0 * eighth
        planes = [
            part(0, 0, 1.0) + sixth * (1.0 / 32.0) - eighth * (1.0 / 128.0),
            part(-2, 0, -2.0) + seventh * (7.0 / 64.0),
            part(1, 1, 1.0) + part(0, 2, -2.0) + eighth * 0.25 - sixth * 0.5625,
            part(-2, 2, 2.0) + part(-4, 0, 2.0) - seventh * 0.875,
            part(2, 2, 1.0) + part(0, 4, 2.0) + part(1, 3, -2.0) + sixth * 1.5 - eighth * 1.25,
            part(-2, 4, -2.0) + part(-4, 2, -2.0) + seventh * 1.75,
        ]
        if j > 0:
            planes = [
                planes[n] + acc_ref[p, n * ROWS : (n + 1) * ROWS, :] for n in range(PLANES)
            ]
        if j < count - 1:
            for n in range(PLANES):
                acc_ref[p, n * ROWS : (n + 1) * ROWS, :] = planes[n]
        else:
            planes_ref[p] = jnp.concatenate(planes[:PLANES], axis=0).astype(jnp.bfloat16)

    lane = lax.broadcasted_iota(jnp.int32, (8, COLS), 1)
    group = lane // 16

    def packed(tiles):
        total = jnp.zeros((8, COLS), jnp.float32)
        for n, tile in enumerate(tiles):
            moved = pltpu.roll(tile, (8 + 16 * n) % COLS, 1)
            total = jnp.where(group == n, moved, total)
        return total

    def unpacked(merged, n):
        tile = pltpu.roll(merged, (COLS - 8 - 16 * n) % COLS, 1)
        return jnp.where((lane < 8) | (lane >= COLS - 8), tile, 0.0)

    first_half = lax.rem(lane, 16) < 8

    def send_around(rows, whole, strip, near_whole, near_strip, sends, recvs):
        copies = []
        for i, (dr, dc) in enumerate(AROUND):
            if (dc == 0) != rows:
                continue
            if dc == 0:
                source, target = whole, near_whole.at[0 if dr == 1 else 1]
            else:
                slot = (1 - dr) * 2 + (0 if dc == 1 else 1)
                source, target = strip, near_strip.at[slot]
            copy = pltpu.make_async_remote_copy(
                src_ref=source,
                dst_ref=target,
                send_sem=sends.at[i],
                recv_sem=recvs.at[i],
                device_id=around[i],
                device_id_type=MESH,
            )
            copy.start()
            copies.append(copy)
        return copies

    operands = (operand_a, operand_b)
    waves = (wave_a, wave_b)
    build = builder(0, operands[0])

    for step in range(WIN // 16):
        build(step)

    for j in range(count):
        build = builder(j + 1, operands[(j + 1) % 2]) if j + 1 < count else None
        for step in range(WIN // 16):
            if step < 3 * TERMS:
                first(operands[j % 2], step)
            if build is not None:
                build(step)
            if j > 0 and step % 2 == 0:
                gather(j - 1, waves[(j - 1) % 2], step // 2)
            if step in (5, 10, 15):
                second(waves[j % 2], step // 5 - 1)
        if j == EARLY:
            pl.semaphore_wait(barrier, len(peers) + len(around))
            loads["quench"].wait()
            for k in range(2):
                own_quench_strip[k] = packed(
                    [quench_ref[r, zh * 8 : zh * 8 + 8, :] for r in range(4 * k, 4 * k + 4) for zh in range(2)]
                )

            quench_copies = []
            for rows in (True, False):
                quench_copies += send_around(
                    rows,
                    quench_ref,
                    own_quench_strip,
                    near_quench,
                    near_quench_strips,
                    quench_send,
                    quench_recv,
                )

    exchange = []
    for d in (4, 5, 3, 6, 2, 7, 1, 0):
        peer = lax.rem(src + d, N_SRC)
        gather(count - 1, waves[(count - 1) % 2], peer)
        if d > 0:
            copy = pltpu.make_async_remote_copy(
                src_ref=planes_ref.at[peer],
                dst_ref=arrived.at[d - 1],
                send_sem=send_sems.at[d - 1],
                recv_sem=recv_sems.at[d - 1],
                device_id=peers[d - 1],
                device_id_type=MESH,
            )
            copy.start()
            exchange.append(copy)

    total = planes_ref[src].astype(jnp.float32)
    for d in range(1, N_SRC):
        exchange[(6, 4, 2, 0, 1, 3, 5)[d - 1]].wait_recv()
        total = total + arrived[d - 1].astype(jnp.float32)
    own_planes[...] = total
    near = (own_planes, own_strip, near_planes, near_strips, near_send, near_recv)
    own_strip[...] = packed([total[n * 8 : n * 8 + 8, :] for n in range(PLANES)])
    strip_copies = send_around(False, *near)
    row_copies = send_around(True, *near)
    plane_copies = row_copies + strip_copies

    for copy in quench_copies:
        copy.wait_recv()
    for g in range(3):
        source = quench_ref if g == 1 else near_quench.at[0 if g == 0 else 1]
        for r in range(8):
            field[1, g * 8 + r, :, 0:COLS] = NEUTRAL * source[r]
        for k in range(2):
            merged = jnp.where(
                first_half, near_quench_strips[2 * g, k], near_quench_strips[2 * g + 1, k]
            )
            for n in range(8):
                row, zh = 4 * k + n // 2, n % 2
                field[1, g * 8 + row, zh * 8 : zh * 8 + 8, COLS : 2 * COLS] = (
                    NEUTRAL * unpacked(merged, n)
                )

    z_at = lax.broadcasted_iota(jnp.int32, (DEPTH, COLS), 0).astype(jnp.float32)
    tau = (z_at - 7.5) * (1.0 / 7.5)
    fading = jnp.exp(-ABSORB * z_at)

    def start_acid(g, get, side):
        for r in range(8):
            value = jnp.broadcast_to(get(PLANES - 1)[r : r + 1], (DEPTH, COLS))
            for n in range(PLANES - 2, -1, -1):
                value = value * tau + get(n)[r : r + 1]
            acid = NEUTRAL - NEUTRAL * jnp.exp(-value * fading)
            field[0, g * 8 + r, :, side * COLS : (side + 1) * COLS] = acid

    start_acid(1, lambda n: own_planes[n * 8 : n * 8 + 8, :], 0)
    for copy in row_copies:
        copy.wait_recv()
    for g in (0, 2):
        start_acid(g, lambda n: near_planes[g // 2, n * 8 : n * 8 + 8, :], 0)
    for copy in strip_copies:
        copy.wait_recv()
    for g in range(3):
        merged = jnp.where(first_half, near_strips[2 * g], near_strips[2 * g + 1])
        tiles = [unpacked(merged, n) for n in range(PLANES)]
        start_acid(g, lambda n: tiles[n], 1)

    for copy in exchange + quench_copies + plane_copies:
        copy.wait_send()


def halo_field(spectra, shift, offset, weights, codes, levels, quench):
    left, right = wave_tables()
    cell_waves, shape_x, shape_y = cell_tables()
    turn = turn_tables()
    bf16, f32, dma = jnp.bfloat16, jnp.float32, pltpu.SemaphoreType.DMA
    vmem, smem = pltpu.VMEM, pltpu.SMEM
    count = spectra.shape[0]
    return pl.pallas_call(
        image_kernel,
        out_shape=jax.ShapeDtypeStruct((2, 3 * ROWS, DEPTH, 2 * COLS), f32),
        in_specs=[pl.BlockSpec(memory_space=pltpu.HBM)] * 13,
        out_specs=pl.BlockSpec(memory_space=pltpu.VMEM),
        scratch_shapes=[
            smem((2, count), jnp.int32),
            smem((2, count), jnp.int32),
            smem(weights.shape, f32),
            smem(levels.shape, f32),
            vmem(codes.shape, jnp.int32),
            vmem(cell_waves.shape, bf16),
            vmem(shape_x.shape, f32),
            vmem(shape_y.shape, f32),
            vmem(turn.shape, f32),
            vmem(left.shape[1:], bf16),
            vmem(right.shape[1:], bf16),
            vmem((2 * N_SRC * ROWS, 2 * WIN), bf16),
            vmem((2 * WIN, 2 * COLS), bf16),
            vmem(spectra.shape, bf16),
            vmem(quench.shape, f32),
            vmem((2, 2 * CELLS, CELLS), f32),
            vmem((3 * TERMS, 2 * WIN, WIN), bf16),
            vmem((3 * TERMS, 2 * WIN, WIN), bf16),
            vmem((3 * TERMS * 64, 2 * WIN), bf16),
            vmem((3 * TERMS * 64, 2 * COLS), f32),
            vmem((3 * TERMS * 64, 2 * COLS), f32),
            vmem((N_SRC, PLANES * ROWS, COLS), f32),
            vmem((N_SRC, PLANES * ROWS, COLS), bf16),
            vmem((N_SRC - 1, PLANES * ROWS, COLS), bf16),
            vmem((PLANES * ROWS, COLS), f32),
            vmem((8, COLS), f32),
            vmem((2, 8, COLS), f32),
            vmem((2, PLANES * ROWS, COLS), f32),
            vmem((6, 8, COLS), f32),
            vmem((2, ROWS, DEPTH, COLS), f32),
            vmem((6, 2, 8, COLS), f32),
            dma((12,)),
            dma((count,)),
            dma((7,)),
            dma((7,)),
            dma((8,)),
            dma((8,)),
            dma((8,)),
            dma((8,)),
        ],
        compiler_params=pltpu.CompilerParams(
            collective_id=0, has_side_effects=True, vmem_limit_bytes=40 << 20
        ),
        name="image",
    )(*(pltpu.with_memory_space_constraint(value, pltpu.HBM) for value in (
        shift.T,
        offset.T,
        weights,
        levels,
        codes,
        jnp.asarray(cell_waves, bf16),
        jnp.asarray(shape_x),
        jnp.asarray(shape_y),
        jnp.asarray(turn),
        jnp.asarray(left, bf16),
        jnp.asarray(right, bf16),
        spectra,
        quench,
    )))


def bake_kernel(start, acid_hbm, quench_hbm, inhibit_hbm, field, acid_out, quench_out, inhibit_out, sems):
    shape = (DEPTH // 2, COLS)
    lane = lax.broadcasted_iota(jnp.int32, shape, 1)
    depth = lax.broadcasted_iota(jnp.int32, shape, 0)
    first_lane, last_lane = lane == 0, lane == COLS - 1
    top, bottom = depth == 0, depth == DEPTH // 2 - 1

    def halves(held, which, row):
        return [
            [held[which, row, z : z + 8, t : t + COLS] for t in (0, COLS)] for z in (0, 8)
        ]

    def sums(held, which, row, sides):
        before, here, after = (halves(held, which, row + k) for k in (-1, 0, 1))
        out = []
        for t in range(sides):
            low, high = here[0][t], here[1][t]
            low_up, high_up = pltpu.roll(low, 1, 0), pltpu.roll(high, 1, 0)
            low_down, high_down = pltpu.roll(low, 7, 0), pltpu.roll(high, 7, 0)
            along = (
                jnp.where(top, low, low_up) + jnp.where(bottom, high_down, low_down),
                jnp.where(top, low_up, high_up) + jnp.where(bottom, high, high_down),
            )
            for z in range(2):
                mine, other = here[z][t], here[z][1 - t]
                left = jnp.where(first_lane, pltpu.roll(other, 1, 1), pltpu.roll(mine, 1, 1))
                right = jnp.where(
                    last_lane, pltpu.roll(other, COLS - 1, 1), pltpu.roll(mine, COLS - 1, 1)
                )
                beside = (before[z][t] + after[z][t]) + (left + right)
                out.append((z, t, mine, beside + 0.25 * along[z]))
        return out

    copies = []

    def send(part):
        rows = pl.ds(part * 4, 4)
        for i, (source, target) in enumerate(
            ((acid_out, acid_hbm), (quench_out, quench_hbm), (inhibit_out, inhibit_hbm))
        ):
            copy = pltpu.make_async_copy(
                source.at[rows], target.at[rows], sems.at[part * 3 + i]
            )
            copy.start()
            copies.append(copy)

    spent = {}
    for step in range(STEPS):
        old = start if step == 0 else field.at[step % 2]
        new = field.at[1 - step % 2]
        last = step == STEPS - 1
        for row in range(step + 1, 23 - step):
            sides = 1 if last or row in (step + 1, 22 - step) else 2
            own = row - 8
            for (z, t, a, a_sum), (_, _, q, q_sum) in zip(
                sums(old, 0, row, sides), sums(old, 1, row, sides)
            ):
                a_new = a * (0.1 - q) + 0.2 * a_sum
                q_new = q * (0.73 - a) + 0.06 * q_sum
                span = slice(z * 8, z * 8 + 8)
                if 0 <= own < ROWS and t == 0:
                    spent[own, z] = spent[own, z] + a if step else a
                if last:
                    acid_out[own, span] = a_new * (1.0 / NEUTRAL)
                    quench_out[own, span] = q_new * (1.0 / NEUTRAL)
                    inhibit_out[own, span] = jnp.exp((-0.25 / NEUTRAL) * spent[own, z])
                else:
                    lanes = slice(t * COLS, (t + 1) * COLS)
                    new[0, row, span, lanes] = a_new
                    new[1, row, span, lanes] = q_new
            if last and own % 4 == 3:
                send(own // 4)

    for copy in copies:
        copy.wait()


def baked(start):
    tile = (ROWS, DEPTH, COLS)
    out = jax.ShapeDtypeStruct(tile, jnp.float32)
    return pl.pallas_call(
        bake_kernel,
        out_shape=(out, out, out),
        in_specs=[pl.BlockSpec(memory_space=pltpu.VMEM)],
        out_specs=(pl.BlockSpec(memory_space=pltpu.HBM),) * 3,
        scratch_shapes=[
            pltpu.VMEM((2, 2, 24, DEPTH, 2 * COLS), jnp.float32),
            pltpu.VMEM(tile, jnp.float32),
            pltpu.VMEM(tile, jnp.float32),
            pltpu.VMEM(tile, jnp.float32),
            pltpu.SemaphoreType.DMA((6,)),
        ],
        compiler_params=pltpu.CompilerParams(vmem_limit_bytes=16 << 20),
        name="bake",
    )(start)


def per_device(
    spectra, pupil_shift, window_offset, source_weight, mask_codes, levels, quench_start
):
    return baked(
        halo_field(
            spectra,
            pupil_shift,
            window_offset,
            source_weight,
            mask_codes,
            levels,
            quench_start,
        )
    )


def solution(mesh):
    in_specs = (
        P("src", None, None, None, None),
        P("src", None),
        P("src", None),
        P(),
        P(),
        P(),
        P(("src", "tx"), None, "ty"),
    )
    out_specs = (
        P(("src", "tx"), None, "ty"),
        P(("src", "tx"), None, "ty"),
        P(("src", "tx"), None, "ty"),
    )
    return jax.shard_map(
        per_device, mesh=mesh, in_specs=in_specs, out_specs=out_specs, check_vma=False
    )
```

```python
import functools
import math

import jax
import jax.numpy as jnp
import numpy as np
from jax import lax
from jax.experimental import pallas as pl
from jax.experimental.pallas import tpu as pltpu
from jax.sharding import PartitionSpec as P

RADIUS = 124
CELL = 4
STEPS = 8
NX = 512
NY = 512
WIN = 256
DEPTH = 16
N_SRC, N_TX, N_TY = 8, 8, 4
ROWS, COLS = 8, 128
CELLS = 128

TWO_PI = 2.0 * math.pi
NUM_AP = 0.33
DZ_WAVE = 0.148
ABSORB = 0.05
NEUTRAL = 0.08

HALF = math.pi * DZ_WAVE * (1.0 - math.sqrt(1.0 - NUM_AP * NUM_AP))
REACH = HALF * 7.5
TERMS = 5
EARLY = 0
REACH_OFF = 3
PLANES = 6
MESH = pl.DeviceIdType.MESH


def fit(function, powers, reach):
    nodes = np.cos((2 * np.arange(400) + 1) * np.pi / 800)
    basis = np.stack([nodes**k for k in powers], 1)
    sides = np.linalg.lstsq(basis, function(reach * nodes), rcond=None)[0]
    return [float(v) for v in sides]


EVEN = fit(np.cos, (0, 2, 4), REACH)
ODD = fit(np.sin, (1, 3), REACH)
SCALE = [EVEN[0], ODD[0], -EVEN[1], -ODD[1], EVEN[2]]


def wave_tables():
    u = np.arange(WIN)
    left = np.zeros((N_TX, 2, N_SRC * ROWS, WIN))
    for tx in range(N_TX):
        local = np.arange(N_SRC * ROWS)
        x = (local // ROWS * N_TX + tx) * ROWS + local % ROWS
        angle = TWO_PI / NX * ((x[:, None] * (u[None, :] - WIN // 2)) % NX)
        c, s = np.cos(angle), np.sin(angle)
        left[tx] = np.stack([c, s])
    right = np.zeros((N_TY, 2, WIN, COLS))
    for ty in range(N_TY):
        y = ty * COLS + np.arange(COLS)
        angle = TWO_PI / NY * ((y[None, :] * (u[:, None] - WIN // 2)) % NY)
        c, s = np.cos(angle), np.sin(angle)
        right[ty] = np.stack([c, s])
    return left, right


def turn_tables():
    fx = np.arange(WIN + 8) - WIN // 2 - REACH_OFF
    fy = np.arange(WIN + 128) - WIN // 2 - REACH_OFF
    radial = fx[:, None] ** 2 + fy[None, :] ** 2
    limit = RADIUS * RADIUS
    axial = np.sqrt(1.0 - (NUM_AP / RADIUS) ** 2 * np.minimum(radial, limit))
    w = TWO_PI * DZ_WAVE * (axial - 1.0) / HALF + 1.0
    inside = radial <= limit
    turn = 8.0 * HALF * w
    table = np.stack([w, np.cos(turn) * inside, np.sin(turn) * inside])
    return np.stack(np.split(table, 3, axis=2), 1).astype(np.float32)


def cell_tables():
    a = np.arange(CELLS)
    angle = TWO_PI / CELLS * ((a[:, None] * a[None, :]) % CELLS)
    c, s = np.cos(angle), np.sin(angle)
    waves = np.stack([c, s]).astype(np.float32)
    high = waves.astype(jnp.bfloat16).astype(np.float32)
    cell_waves = np.stack([high, waves - high])
    orders = np.arange(NX) - NX // 2
    phase = TWO_PI / NX * ((orders[:, None] * np.arange(CELL)[None, :]) % NX)
    shape_re = np.cos(phase).sum(1) / NX
    shape_im = -np.sin(phase).sum(1) / NX
    shape = np.stack([shape_re, shape_im])
    shape_x = np.broadcast_to(shape[:, :, None], (2, NX, 128))
    shape_y = np.broadcast_to(shape[:, None, :], (2, 8, NY))
    return (
        cell_waves,
        shape_x.astype(np.float32),
        shape_y.astype(np.float32),
    )


AROUND = [(-1, -1), (-1, 1), (1, -1), (1, 1), (0, -1), (0, 1), (-1, 0), (1, 0)]


def image_kernel(
    shift_hbm,
    offset_hbm,
    weight_hbm,
    levels_hbm,
    codes_hbm,
    cell_waves_hbm,
    shape_x_hbm,
    shape_y_hbm,
    turn_hbm,
    left_hbm,
    right_hbm,
    spectra_hbm,
    quench_hbm,
    field,
    shift_ref,
    offset_ref,
    weight_ref,
    levels_ref,
    codes_ref,
    cell_waves_ref,
    shape_x_ref,
    shape_y_ref,
    turn_ref,
    left_in,
    right_in,
    left_ref,
    right_ref,
    spectra_ref,
    quench_ref,
    cells_ref,
    operand_a,
    operand_b,
    half_ref,
    wave_a,
    wave_b,
    acc_ref,
    planes_ref,
    arrived,
    own_planes,
    own_strip,
    own_quench_strip,
    near_planes,
    near_strips,
    near_quench,
    near_quench_strips,
    load_sems,
    spectra_sems,
    send_sems,
    recv_sems,
    near_send,
    near_recv,
    quench_send,
    quench_recv,
):
    src, tx, ty = lax.axis_index("src"), lax.axis_index("tx"), lax.axis_index("ty")
    place = src * N_TX + tx

    def device_at(dr, dc):
        row = lax.rem(place + dr + N_SRC * N_TX, N_SRC * N_TX)
        column = lax.rem(ty + dc + N_TY, N_TY)
        return (row // N_TX, lax.rem(row, N_TX), column)

    peers = [(lax.rem(src + d, N_SRC), tx, ty) for d in range(1, N_SRC)]
    around = [device_at(dr, dc) for dr, dc in AROUND]

    loads = {}
    pairs = [
        ("codes", codes_hbm, codes_ref),
        ("levels", levels_hbm, levels_ref),
        ("cell", cell_waves_hbm, cell_waves_ref),
        ("shift", shift_hbm, shift_ref),
        ("offset", offset_hbm, offset_ref),
        ("weight", weight_hbm, weight_ref),
        ("shape_x", shape_x_hbm, shape_x_ref),
        ("shape_y", shape_y_hbm, shape_y_ref),
        ("turn", turn_hbm, turn_ref),
        ("left", left_hbm.at[tx], left_in),
        ("right", right_hbm.at[ty], right_in),
        ("quench", quench_hbm, quench_ref),
    ]
    count = spectra_hbm.shape[0]
    spectra_loads = [
        pltpu.make_async_copy(spectra_hbm.at[j], spectra_ref.at[j], spectra_sems.at[j])
        for j in range(count)
    ]
    for i, (name, source, target) in enumerate(pairs):
        loads[name] = pltpu.make_async_copy(source, target, load_sems.at[i])
        loads[name].start()
        if name == "turn":
            spectra_loads[0].start()
    for copy in spectra_loads[1:]:
        copy.start()

    barrier = pltpu.get_barrier_semaphore()
    for device in peers + around:
        pl.semaphore_signal(barrier, inc=1, device_id=device, device_id_type=MESH)

    for name in ("codes", "levels", "cell"):
        loads[name].wait()
    codes = codes_ref[...]
    parts = []
    for part in range(2):
        grid = jnp.full(codes.shape, levels_ref[part, 3], jnp.float32)
        for level in range(3):
            grid = jnp.where(codes == level, levels_ref[part, level], grid)
        parts.append(grid)
    by_column, by_row = [], []
    for part in range(2):
        c, s = cell_waves_ref[part, 0], cell_waves_ref[part, 1]
        by_column.append(
            jnp.concatenate(
                [jnp.concatenate([c, -s], axis=1), jnp.concatenate([s, c], axis=1)], axis=0
            )
        )
        by_row.append(
            jnp.concatenate(
                [jnp.concatenate([c, s], axis=1), jnp.concatenate([-s, c], axis=1)], axis=0
            )
        )
    by_column = jnp.concatenate([by_column[0], by_column[0], by_column[1]], axis=0)
    by_row = jnp.concatenate([by_row[0], by_row[0], by_row[1]], axis=1)
    grid = jnp.concatenate(parts, axis=1)
    high = grid.astype(jnp.bfloat16)
    low = (grid - high.astype(jnp.float32)).astype(jnp.bfloat16)
    across = jnp.dot(
        jnp.concatenate([high, low, high], axis=1),
        by_column,
        preferred_element_type=jnp.float32,
    )
    both = jnp.concatenate([across[:, :CELLS], across[:, CELLS:]], axis=0)
    high = both.astype(jnp.bfloat16)
    low = (both - high.astype(jnp.float32)).astype(jnp.bfloat16)
    full = jnp.dot(
        by_row,
        jnp.concatenate([high, low, high], axis=0),
        preferred_element_type=jnp.float32,
    )
    for part in range(2):
        piece = full[part * CELLS : (part + 1) * CELLS]
        cells_ref[part, 0:CELLS] = piece
        cells_ref[part, CELLS : 2 * CELLS] = piece
    for name in ("shift", "offset", "weight", "shape_x", "shape_y", "turn", "left", "right"):
        loads[name].wait()

    rows = N_SRC * ROWS
    left_ref[0:rows, 0:WIN] = left_in[0]
    left_ref[0:rows, WIN : 2 * WIN] = -left_in[1]
    left_ref[rows : 2 * rows, 0:WIN] = left_in[1]
    left_ref[rows : 2 * rows, WIN : 2 * WIN] = left_in[0]
    right_ref[0:WIN, 0:COLS] = right_in[0]
    right_ref[0:WIN, COLS : 2 * COLS] = right_in[1]
    right_ref[WIN : 2 * WIN, 0:COLS] = -right_in[1]
    right_ref[WIN : 2 * WIN, COLS : 2 * COLS] = right_in[0]

    total_weight = weight_ref[0]
    for k in range(1, weight_ref.shape[0]):
        total_weight = total_weight + weight_ref[k]
    norm = 1.0 / jnp.full((ROWS, COLS), total_weight, jnp.float32)

    def builder(j, operand):
        spectra_loads[j].wait()
        off_x, off_y = offset_ref[0, j], offset_ref[1, j]
        start_x = off_x - shift_ref[0, j] - WIN // 2 + NX // 2
        start_y = off_y - shift_ref[1, j] - WIN // 2 + NY // 2
        cell_x = lax.rem(start_x, CELLS)
        roll_y = lax.rem(2 * CELLS - lax.rem(start_y, CELLS), CELLS)
        turn_x = off_x + REACH_OFF
        turn_y = lax.rem(COLS - (off_y + REACH_OFF), COLS)
        shape_y = [
            pltpu.roll(shape_y_ref[part], NY - start_y, 1)[:, :WIN] for part in range(2)
        ]
        y_both = [jnp.concatenate([value] * 2, axis=0) for value in shape_y]

        lane = lax.broadcasted_iota(jnp.int32, (16, COLS), 1)
        kept = lane < COLS - (off_y + REACH_OFF)

        def turned(k, at):
            moved = [
                pltpu.roll(turn_ref[k, t, pl.ds(turn_x + at, 16), :], turn_y, 1)
                for t in range(3)
            ]
            return [jnp.where(kept, moved[t], moved[t + 1]) for t in range(2)]

        def build(step):
            at = step * 16 if isinstance(step, int) else pl.multiple_of(step * 16, 16)
            cell_at = lax.rem(cell_x + at, CELLS)
            g_re = pltpu.roll(cells_ref[0, pl.ds(cell_at, 16), :], roll_y, 1)
            g_im = pltpu.roll(cells_ref[1, pl.ds(cell_at, 16), :], roll_y, 1)
            x_re = shape_x_ref[0, pl.ds(start_x + at, 16), :]
            x_im = shape_x_ref[1, pl.ds(start_x + at, 16), :]
            gx_re = g_re * x_re - g_im * x_im
            gx_im = g_re * x_im + g_im * x_re
            w_both, turn_re_both, turn_im_both = (turned(k, at) for k in range(3))
            w = jnp.concatenate(w_both, axis=1).astype(jnp.bfloat16)
            turn_re = jnp.concatenate(turn_re_both, axis=1)
            turn_im = jnp.concatenate(turn_im_both, axis=1)
            gx_re = jnp.concatenate([gx_re, gx_re], axis=1)
            gx_im = jnp.concatenate([gx_im, gx_im], axis=1)
            y_re, y_im = y_both
            thin_re = gx_re * y_re - gx_im * y_im
            thin_im = gx_re * y_im + gx_im * y_re
            h_re = thin_re * turn_re - thin_im * turn_im
            h_im = thin_re * turn_im + thin_im * turn_re
            for c in range(3):
                f_re = spectra_ref[j, c, 0, pl.ds(at, 16), :].astype(jnp.float32)
                f_im = spectra_ref[j, c, 1, pl.ds(at, 16), :].astype(jnp.float32)
                s_re = (f_re * h_re - f_im * h_im).astype(jnp.bfloat16)
                s_im = (f_re * h_im + f_im * h_re).astype(jnp.bfloat16)
                for n in range(TERMS):
                    operand[c * TERMS + n, pl.ds(at, 16), :] = s_re
                    operand[c * TERMS + n, pl.ds(WIN + at, 16), :] = s_im
                    if n < TERMS - 1:
                        s_re = s_re * w
                        s_im = s_im * w

        return build

    def first(operand, block):
        halves = jnp.dot(
            left_ref[...], operand[block], preferred_element_type=jnp.float32
        ).astype(jnp.bfloat16)
        half_ref[block * 64 : (block + 1) * 64, 0:WIN] = halves[0:64]
        half_ref[block * 64 : (block + 1) * 64, WIN : 2 * WIN] = halves[64:128]

    def second(wave, c):
        span = slice(c * TERMS * 64, (c + 1) * TERMS * 64)
        wave[span, :] = jnp.dot(
            half_ref[span, :], right_ref[...], preferred_element_type=jnp.float32
        )

    def gather(j, wave, p, parts=(0, 1, 2)):
        at = p * ROWS
        final = j == count - 1 and parts[-1] == 2
        if final:
            at = pl.multiple_of(at, ROWS)
        weight = weight_ref[src * count + j] * norm
        real = ((0, 0), (1, 1), (0, 2), (2, 2), (0, 4), (1, 3), (3, 3), (2, 4), (4, 4))
        imag = ((1, 0), (1, 2), (3, 0), (1, 4), (3, 2), (3, 4))
        total = {}
        for c in parts:
            re, im = [], []
            for n in range(TERMS):
                rows = pl.ds((c * TERMS + n) * 64 + at, ROWS)
                re.append(wave[rows, 0:COLS])
                im.append(wave[rows, COLS : 2 * COLS])
            for a, b in real:
                value = re[a] * re[b] + im[a] * im[b]
                total[a, b] = value if c == parts[0] else total[a, b] + value
            for a, b in imag:
                value = im[a] * re[b] - re[a] * im[b]
                total[-a - 1, b] = value if c == parts[0] else total[-a - 1, b] + value

        def part(a, b, factor):
            sign = a if a >= 0 else -a - 1
            return total[a, b] * (weight * (factor * SCALE[sign] * SCALE[b]))

        eighth = part(4, 4, 1.0)
        seventh = part(-4, 4, 2.0)
        sixth = part(3, 3, 1.0) + part(2, 4, -2.0) + 2.0 * eighth
        planes = [
            part(0, 0, 1.0) + sixth * (1.0 / 32.0) - eighth * (1.0 / 128.0),
            part(-2, 0, -2.0) + seventh * (7.0 / 64.0),
            part(1, 1, 1.0) + part(0, 2, -2.0) + eighth * 0.25 - sixth * 0.5625,
            part(-2, 2, 2.0) + part(-4, 0, 2.0) - seventh * 0.875,
            part(2, 2, 1.0) + part(0, 4, 2.0) + part(1, 3, -2.0) + sixth * 1.5 - eighth * 1.25,
            part(-2, 4, -2.0) + part(-4, 2, -2.0) + seventh * 1.75,
        ]
        if j > 0:
            planes = [
                planes[n] + acc_ref[p, n * ROWS : (n + 1) * ROWS, :] for n in range(PLANES)
            ]
        if not final:
            for n in range(PLANES):
                acc_ref[p, n * ROWS : (n + 1) * ROWS, :] = planes[n]
        else:
            planes_ref[p] = jnp.concatenate(planes[:PLANES], axis=0).astype(jnp.bfloat16)

    lane = lax.broadcasted_iota(jnp.int32, (8, COLS), 1)
    group = lane // 16

    def packed(tiles):
        total = jnp.zeros((8, COLS), jnp.float32)
        for n, tile in enumerate(tiles):
            moved = pltpu.roll(tile, (8 + 16 * n) % COLS, 1)
            total = jnp.where(group == n, moved, total)
        return total

    def unpacked(merged, n):
        tile = pltpu.roll(merged, (COLS - 8 - 16 * n) % COLS, 1)
        return jnp.where((lane < 8) | (lane >= COLS - 8), tile, 0.0)

    first_half = lax.rem(lane, 16) < 8

    def send_around(rows, whole, strip, near_whole, near_strip, sends, recvs):
        copies = []
        for i, (dr, dc) in enumerate(AROUND):
            if (dc == 0) != rows:
                continue
            if dc == 0:
                source, target = whole, near_whole.at[0 if dr == 1 else 1]
            else:
                slot = (1 - dr) * 2 + (0 if dc == 1 else 1)
                source, target = strip, near_strip.at[slot]
            copy = pltpu.make_async_remote_copy(
                src_ref=source,
                dst_ref=target,
                send_sem=sends.at[i],
                recv_sem=recvs.at[i],
                device_id=around[i],
                device_id_type=MESH,
            )
            copy.start()
            copies.append(copy)
        return copies

    operands = (operand_a, operand_b)
    waves = (wave_a, wave_b)
    build = builder(0, operands[0])

    for step in range(WIN // 16):
        build(step)

    for j in range(count):
        build = builder(j + 1, operands[(j + 1) % 2]) if j + 1 < count else None
        for step in range(WIN // 16):
            if step < 3 * TERMS:
                first(operands[j % 2], step)
            if build is not None:
                build(step)
            if j > 0 and step % 2 == 0:
                gather(j - 1, waves[(j - 1) % 2], step // 2)
            if step in (5, 10, 15):
                second(waves[j % 2], step // 5 - 1)
            if j == count - 1 and step > 10:
                for p in range(8 * (step - 11) // 5, 8 * (step - 10) // 5):
                    gather(j, waves[j % 2], p, (0, 1))
        if j == EARLY:
            pl.semaphore_wait(barrier, len(peers) + len(around))
            loads["quench"].wait()
            for k in range(2):
                own_quench_strip[k] = packed(
                    [quench_ref[r, zh * 8 : zh * 8 + 8, :] for r in range(4 * k, 4 * k + 4) for zh in range(2)]
                )

            quench_copies = []
            for rows in (True, False):
                quench_copies += send_around(
                    rows,
                    quench_ref,
                    own_quench_strip,
                    near_quench,
                    near_quench_strips,
                    quench_send,
                    quench_recv,
                )

    exchange = []
    for d in (4, 5, 3, 6, 2, 7, 1, 0):
        peer = lax.rem(src + d, N_SRC)
        gather(count - 1, waves[(count - 1) % 2], peer, (2,))
        if d > 0:
            copy = pltpu.make_async_remote_copy(
                src_ref=planes_ref.at[peer],
                dst_ref=arrived.at[d - 1],
                send_sem=send_sems.at[d - 1],
                recv_sem=recv_sems.at[d - 1],
                device_id=peers[d - 1],
                device_id_type=MESH,
            )
            copy.start()
            exchange.append(copy)

    total = planes_ref[src].astype(jnp.float32)
    for d in range(1, N_SRC):
        exchange[(6, 4, 2, 0, 1, 3, 5)[d - 1]].wait_recv()
        total = total + arrived[d - 1].astype(jnp.float32)
    own_planes[...] = total
    near = (own_planes, own_strip, near_planes, near_strips, near_send, near_recv)
    own_strip[...] = packed([total[n * 8 : n * 8 + 8, :] for n in range(PLANES)])
    strip_copies = send_around(False, *near)
    row_copies = send_around(True, *near)
    plane_copies = row_copies + strip_copies

    for copy in quench_copies:
        copy.wait_recv()
    for g in range(3):
        source = quench_ref if g == 1 else near_quench.at[0 if g == 0 else 1]
        for r in range(8):
            field[1, g * 8 + r, :, 0:COLS] = NEUTRAL * source[r]
        for k in range(2):
            merged = jnp.where(
                first_half, near_quench_strips[2 * g, k], near_quench_strips[2 * g + 1, k]
            )
            for n in range(8):
                row, zh = 4 * k + n // 2, n % 2
                field[1, g * 8 + row, zh * 8 : zh * 8 + 8, COLS : 2 * COLS] = (
                    NEUTRAL * unpacked(merged, n)
                )

    z_at = lax.broadcasted_iota(jnp.int32, (DEPTH, COLS), 0).astype(jnp.float32)
    tau = (z_at - 7.5) * (1.0 / 7.5)
    fading = jnp.exp(-ABSORB * z_at)

    def start_acid(g, get, side):
        for r in range(8):
            value = jnp.broadcast_to(get(PLANES - 1)[r : r + 1], (DEPTH, COLS))
            for n in range(PLANES - 2, -1, -1):
                value = value * tau + get(n)[r : r + 1]
            acid = NEUTRAL - NEUTRAL * jnp.exp(-value * fading)
            field[0, g * 8 + r, :, side * COLS : (side + 1) * COLS] = acid

    start_acid(1, lambda n: own_planes[n * 8 : n * 8 + 8, :], 0)
    for g in (0, 2):
        row_copies[0 if g == 2 else 1].wait_recv()
        start_acid(g, lambda n: near_planes[g // 2, n * 8 : n * 8 + 8, :], 0)
    corners = [shift for shift in AROUND if shift[1] != 0]
    for g in (1, 0, 2):
        for (dr, _), copy in zip(corners, strip_copies):
            if 1 - dr == g:
                copy.wait_recv()
        merged = jnp.where(first_half, near_strips[2 * g], near_strips[2 * g + 1])
        tiles = [unpacked(merged, n) for n in range(PLANES)]
        start_acid(g, lambda n: tiles[n], 1)

    for copy in exchange + quench_copies + plane_copies:
        copy.wait_send()


def halo_field(spectra, shift, offset, weights, codes, levels, quench):
    left, right = wave_tables()
    cell_waves, shape_x, shape_y = cell_tables()
    turn = turn_tables()
    bf16, f32, dma = jnp.bfloat16, jnp.float32, pltpu.SemaphoreType.DMA
    vmem, smem = pltpu.VMEM, pltpu.SMEM
    count = spectra.shape[0]
    return pl.pallas_call(
        image_kernel,
        out_shape=jax.ShapeDtypeStruct((2, 3 * ROWS, DEPTH, 2 * COLS), f32),
        in_specs=[pl.BlockSpec(memory_space=pltpu.HBM)] * 13,
        out_specs=pl.BlockSpec(memory_space=pltpu.VMEM),
        scratch_shapes=[
            smem((2, count), jnp.int32),
            smem((2, count), jnp.int32),
            smem(weights.shape, f32),
            smem(levels.shape, f32),
            vmem(codes.shape, jnp.int32),
            vmem(cell_waves.shape, bf16),
            vmem(shape_x.shape, f32),
            vmem(shape_y.shape, f32),
            vmem(turn.shape, f32),
            vmem(left.shape[1:], bf16),
            vmem(right.shape[1:], bf16),
            vmem((2 * N_SRC * ROWS, 2 * WIN), bf16),
            vmem((2 * WIN, 2 * COLS), bf16),
            vmem(spectra.shape, bf16),
            vmem(quench.shape, f32),
            vmem((2, 2 * CELLS, CELLS), f32),
            vmem((3 * TERMS, 2 * WIN, WIN), bf16),
            vmem((3 * TERMS, 2 * WIN, WIN), bf16),
            vmem((3 * TERMS * 64, 2 * WIN), bf16),
            vmem((3 * TERMS * 64, 2 * COLS), f32),
            vmem((3 * TERMS * 64, 2 * COLS), f32),
            vmem((N_SRC, PLANES * ROWS, COLS), f32),
            vmem((N_SRC, PLANES * ROWS, COLS), bf16),
            vmem((N_SRC - 1, PLANES * ROWS, COLS), bf16),
            vmem((PLANES * ROWS, COLS), f32),
            vmem((8, COLS), f32),
            vmem((2, 8, COLS), f32),
            vmem((2, PLANES * ROWS, COLS), f32),
            vmem((6, 8, COLS), f32),
            vmem((2, ROWS, DEPTH, COLS), f32),
            vmem((6, 2, 8, COLS), f32),
            dma((12,)),
            dma((count,)),
            dma((7,)),
            dma((7,)),
            dma((8,)),
            dma((8,)),
            dma((8,)),
            dma((8,)),
        ],
        compiler_params=pltpu.CompilerParams(
            collective_id=0, has_side_effects=True, vmem_limit_bytes=40 << 20
        ),
        name="image",
    )(*(pltpu.with_memory_space_constraint(value, pltpu.HBM) for value in (
        shift.T,
        offset.T,
        weights,
        levels,
        codes,
        jnp.asarray(cell_waves, bf16),
        jnp.asarray(shape_x),
        jnp.asarray(shape_y),
        jnp.asarray(turn),
        jnp.asarray(left, bf16),
        jnp.asarray(right, bf16),
        spectra,
        quench,
    )))


def bake_kernel(start, acid_hbm, quench_hbm, inhibit_hbm, field, acid_out, quench_out, inhibit_out, sems):
    shape = (DEPTH // 2, COLS)
    lane = lax.broadcasted_iota(jnp.int32, shape, 1)
    depth = lax.broadcasted_iota(jnp.int32, shape, 0)
    first_lane, last_lane = lane == 0, lane == COLS - 1
    top, bottom = depth == 0, depth == DEPTH // 2 - 1

    def halves(held, which, row):
        return [
            [held[which, row, z : z + 8, t : t + COLS] for t in (0, COLS)] for z in (0, 8)
        ]

    def sums(held, which, row, sides):
        before, here, after = (halves(held, which, row + k) for k in (-1, 0, 1))
        out = []
        for t in range(sides):
            low, high = here[0][t], here[1][t]
            low_up, high_up = pltpu.roll(low, 1, 0), pltpu.roll(high, 1, 0)
            low_down, high_down = pltpu.roll(low, 7, 0), pltpu.roll(high, 7, 0)
            along = (
                jnp.where(top, low, low_up) + jnp.where(bottom, high_down, low_down),
                jnp.where(top, low_up, high_up) + jnp.where(bottom, high, high_down),
            )
            for z in range(2):
                mine, other = here[z][t], here[z][1 - t]
                left = jnp.where(first_lane, pltpu.roll(other, 1, 1), pltpu.roll(mine, 1, 1))
                right = jnp.where(
                    last_lane, pltpu.roll(other, COLS - 1, 1), pltpu.roll(mine, COLS - 1, 1)
                )
                beside = (before[z][t] + after[z][t]) + (left + right)
                out.append((z, t, mine, beside + 0.25 * along[z]))
        return out

    copies = []

    def send(part):
        rows = pl.ds(part * 4, 4)
        for i, (source, target) in enumerate(
            ((acid_out, acid_hbm), (quench_out, quench_hbm), (inhibit_out, inhibit_hbm))
        ):
            copy = pltpu.make_async_copy(
                source.at[rows], target.at[rows], sems.at[part * 3 + i]
            )
            copy.start()
            copies.append(copy)

    spent = {}
    for step in range(STEPS):
        old = start if step == 0 else field.at[step % 2]
        new = field.at[1 - step % 2]
        last = step == STEPS - 1
        for row in range(step + 1, 23 - step):
            sides = 1 if last or row in (step + 1, 22 - step) else 2
            own = row - 8
            for (z, t, a, a_sum), (_, _, q, q_sum) in zip(
                sums(old, 0, row, sides), sums(old, 1, row, sides)
            ):
                a_new = a * (0.1 - q) + 0.2 * a_sum
                q_new = q * (0.73 - a) + 0.06 * q_sum
                span = slice(z * 8, z * 8 + 8)
                if 0 <= own < ROWS and t == 0:
                    spent[own, z] = spent[own, z] + a if step else a
                if last:
                    acid_out[own, span] = a_new * (1.0 / NEUTRAL)
                    quench_out[own, span] = q_new * (1.0 / NEUTRAL)
                    inhibit_out[own, span] = jnp.exp((-0.25 / NEUTRAL) * spent[own, z])
                else:
                    lanes = slice(t * COLS, (t + 1) * COLS)
                    new[0, row, span, lanes] = a_new
                    new[1, row, span, lanes] = q_new
            if last and own % 4 == 3:
                send(own // 4)

    for copy in copies:
        copy.wait()


def baked(start):
    tile = (ROWS, DEPTH, COLS)
    out = jax.ShapeDtypeStruct(tile, jnp.float32)
    return pl.pallas_call(
        bake_kernel,
        out_shape=(out, out, out),
        in_specs=[pl.BlockSpec(memory_space=pltpu.VMEM)],
        out_specs=(pl.BlockSpec(memory_space=pltpu.HBM),) * 3,
        scratch_shapes=[
            pltpu.VMEM((2, 2, 24, DEPTH, 2 * COLS), jnp.float32),
            pltpu.VMEM(tile, jnp.float32),
            pltpu.VMEM(tile, jnp.float32),
            pltpu.VMEM(tile, jnp.float32),
            pltpu.SemaphoreType.DMA((6,)),
        ],
        compiler_params=pltpu.CompilerParams(vmem_limit_bytes=16 << 20),
        name="bake",
    )(start)


def per_device(
    spectra, pupil_shift, window_offset, source_weight, mask_codes, levels, quench_start
):
    return baked(
        halo_field(
            spectra,
            pupil_shift,
            window_offset,
            source_weight,
            mask_codes,
            levels,
            quench_start,
        )
    )


def solution(mesh):
    in_specs = (
        P("src", None, None, None, None),
        P("src", None),
        P("src", None),
        P(),
        P(),
        P(),
        P(("src", "tx"), None, "ty"),
    )
    out_specs = (
        P(("src", "tx"), None, "ty"),
        P(("src", "tx"), None, "ty"),
        P(("src", "tx"), None, "ty"),
    )
    return jax.shard_map(
        per_device, mesh=mesh, in_specs=in_specs, out_specs=out_specs, check_vma=False
    )
```
